32 devices in a mesh: cp: 4 (over z), fsdp: 8 (over y, x, core).
Axes of the slice: x: 2, y: 2, z: 4, core: 2. Of those that a mesh axis runs over, the one named last changes fastest.
Arguments:
- tokens: int32 [256, 256], P('fsdp', 'cp')
- lengths: int32 [256], P('fsdp')
- embed_table: bfloat16 [33, 480], replicated
- layer_vecs: float32 [9, 480], P(None, 'fsdp')
- w_qkv: bfloat16 [480, 3, 20, 24], P('fsdp')
- w_out: bfloat16 [480, 480], P('fsdp')
- w_up: bfloat16 [480, 1920], P('fsdp')
- b_up: float32 [1920], P('fsdp')
- w_down: bfloat16 [1920, 480], P('fsdp')
- grad_out: bfloat16 [256, 256, 480], P('fsdp', 'cp')
Outputs:
- output 1: bfloat16 [256, 256, 480], P('fsdp', 'cp')
- output 2: float32 [33, 480], replicated
- output 3: float32 [9, 480], P(None, 'fsdp')
- output 4: float32 [480, 3, 20, 24], P('fsdp')
- output 5: float32 [480, 480], P('fsdp')
- output 6: float32 [480, 1920], P('fsdp')
- output 7: float32 [1920], P('fsdp')
- output 8: float32 [1920, 480], P('fsdp')
All inputs are finite; a program needn't handle non-finite values.
Results may differ from the reference program's by a relative error of at most 0.0101958.
Values are sent between devices in bfloat16 or wider.
A program may use at most 1 GiB of HBM per device.

```python
import jax
import jax.numpy as jnp
from jax import lax

NUM_SEQS = 256
SEQ_LEN = 256
MODEL_DIM = 480
NUM_HEADS = 20
FFN_DIM = 1920
VOCAB_SIZE = 33
BOS_ID = 0
PAD_ID = 1
EOS_ID = 2
MASK_ID = 32
HEAD_DIM = MODEL_DIM // NUM_HEADS
LN_EPS = 1e-5
ROPE_BASE = 10000.0
TRAIN_RATIO = 0.15 * 0.8
NEG_BIG = -1e30


def draw_tokens(rng_key):
    key_list = jax.random.split(rng_key, 4)
    lengths = jax.random.randint(key_list[0], (NUM_SEQS,), SEQ_LEN // 4, SEQ_LEN + 1)
    lengths = lengths.at[0].set(SEQ_LEN).at[1].set(SEQ_LEN // 4)
    positions = jnp.arange(SEQ_LEN)[None, :]
    len_col = lengths[:, None]
    residues = jax.random.randint(key_list[1], (NUM_SEQS, SEQ_LEN), 4, 31)
    win_start = jax.random.randint(key_list[2], (NUM_SEQS, 1), 0, SEQ_LEN)
    in_win = (positions >= win_start) & (positions < win_start + SEQ_LEN // 4)
    hit_draw = jax.random.randint(key_list[3], (NUM_SEQS, SEQ_LEN), 0, 100)
    is_mask = hit_draw < jnp.where(in_win, 45, 5)
    tokens = jnp.where(is_mask, MASK_ID, residues)
    tokens = jnp.where(positions >= len_col, PAD_ID, tokens)
    tokens = jnp.where(positions == len_col - 1, EOS_ID, tokens)
    tokens = jnp.where(positions == 0, BOS_ID, tokens)
    return tokens.astype(jnp.int32), lengths.astype(jnp.int32)


def setup_inputs(seed: int = 0) -> dict:
    key_list = jax.random.split(jax.random.key(seed), 9)
    tokens, lengths = draw_tokens(key_list[0])
    embed_table = jax.random.normal(key_list[1], (VOCAB_SIZE, MODEL_DIM), jnp.float32)
    row_scale = jnp.array([0.2, 0.3, 0.3, 0.3, SEQ_LEN ** -0.5, 0.3, 0.2, 0.3, 0.3], jnp.float32)
    row_shift = jnp.array([1.0, 0.0, 0.0, 0.0, 0.0, 0.0, 1.0, 0.0, 0.0], jnp.float32)
    layer_vecs = row_shift[:, None] + row_scale[:, None] * jax.random.normal(key_list[2], (9, MODEL_DIM), jnp.float32)
    w_qkv = jax.random.normal(key_list[3], (MODEL_DIM, 3, NUM_HEADS, HEAD_DIM), jnp.float32) * MODEL_DIM ** -0.5
    w_out = jax.random.normal(key_list[4], (MODEL_DIM, MODEL_DIM), jnp.float32) * (SEQ_LEN / (2.0 * MODEL_DIM)) ** 0.5
    w_up = jax.random.normal(key_list[5], (MODEL_DIM, FFN_DIM), jnp.float32) * MODEL_DIM ** -0.5
    b_up = 0.5 * jax.random.normal(key_list[6], (FFN_DIM,), jnp.float32)
    w_down = jax.random.normal(key_list[7], (FFN_DIM, MODEL_DIM), jnp.float32) * FFN_DIM ** -0.5
    grad_out = jax.random.normal(key_list[8], (NUM_SEQS, SEQ_LEN, MODEL_DIM), jnp.float32)
    return {
        'tokens': tokens,
        'lengths': lengths,
        'embed_table': embed_table.astype(jnp.bfloat16),
        'layer_vecs': layer_vecs,
        'w_qkv': w_qkv.astype(jnp.bfloat16),
        'w_out': w_out.astype(jnp.bfloat16),
        'w_up': w_up.astype(jnp.bfloat16),
        'b_up': b_up,
        'w_down': w_down.astype(jnp.bfloat16),
        'grad_out': grad_out.astype(jnp.bfloat16),
    }


def rounded(z_in):
    return z_in + lax.stop_gradient(z_in.astype(jnp.bfloat16).astype(jnp.float32) - z_in)


def layer_norm(z_in, ln_gain, ln_bias):
    row_mean = jnp.mean(z_in, axis=-1, keepdims=True)
    centered = z_in - row_mean
    row_var = jnp.mean(centered * centered, axis=-1, keepdims=True)
    return centered * lax.rsqrt(row_var + LN_EPS) * ln_gain + ln_bias


def rotate(z_in, cos_t, sin_t):
    lower_half, upper_half = jnp.split(z_in, 2, axis=-1)
    return jnp.concatenate([lower_half * cos_t - upper_half * sin_t, upper_half * cos_t + lower_half * sin_t], axis=-1)


def one_sequence(params, embed_f32, tok_row, len_row):
    layer_vecs, w_qkv, w_out, w_up, b_up, w_down = params
    positions = jnp.arange(SEQ_LEN)
    is_mask = tok_row == MASK_ID
    key_valid = positions < len_row
    n_mask = jnp.sum(is_mask.astype(jnp.float32))
    drop_scale = (1.0 - TRAIN_RATIO) / (1.0 - n_mask / len_row.astype(jnp.float32))
    keep_scale = jnp.where(is_mask | jnp.logical_not(key_valid), 0.0, drop_scale)
    embedded = embed_f32[tok_row] * keep_scale[:, None]
    norm_in = rounded(layer_norm(embedded, layer_vecs[0], layer_vecs[1]))
    qkv_lin = jnp.dot(norm_in, w_qkv.reshape(MODEL_DIM, 3 * MODEL_DIM)) + layer_vecs[2:5].reshape(3 * MODEL_DIM)
    qkv_lin = qkv_lin.reshape(SEQ_LEN, 3, NUM_HEADS, HEAD_DIM)
    inv_freq = 1.0 / (ROPE_BASE ** (jnp.arange(0, HEAD_DIM, 2, dtype=jnp.float32) / HEAD_DIM))
    angles = positions.astype(jnp.float32)[:, None] * inv_freq[None, :]
    cos_t = jnp.cos(angles)[:, None, :]
    sin_t = jnp.sin(angles)[:, None, :]
    q_heads = rounded(rotate(qkv_lin[:, 0] * HEAD_DIM ** -0.5, cos_t, sin_t))
    k_heads = rounded(rotate(qkv_lin[:, 1], cos_t, sin_t))
    v_heads = rounded(qkv_lin[:, 2])

    def one_head(head_in):
        q_h, k_h, v_h = head_in
        scores = jnp.dot(q_h, k_h.T)
        scores = jnp.where(key_valid[None, :], scores, NEG_BIG)
        return jnp.dot(jax.nn.softmax(scores, axis=-1), v_h)

    per_head = lax.map(jax.checkpoint(one_head), (q_heads.transpose(1, 0, 2), k_heads.transpose(1, 0, 2), v_heads.transpose(1, 0, 2)))
    attn_out = rounded(per_head.transpose(1, 0, 2).reshape(SEQ_LEN, MODEL_DIM))
    resid_mid = embedded + jnp.dot(attn_out, w_out) + layer_vecs[5]
    norm_mid = rounded(layer_norm(resid_mid, layer_vecs[6], layer_vecs[7]))
    gelu_out = rounded(jax.nn.gelu(jnp.dot(norm_mid, w_up) + b_up, approximate=False))
    return resid_mid + jnp.dot(gelu_out, w_down) + layer_vecs[8]


def reference(tokens, lengths, embed_table, layer_vecs, w_qkv, w_out, w_up, b_up, w_down, grad_out):
    params = (layer_vecs, w_qkv.astype(jnp.float32), w_out.astype(jnp.float32), w_up.astype(jnp.float32), b_up, w_down.astype(jnp.float32))
    seq_fn = jax.checkpoint(one_sequence)

    def forward(params_in, embed_f32):
        def per_row(seq_row):
            return seq_fn(params_in, embed_f32, seq_row[0], seq_row[1])
        return lax.map(per_row, (tokens, lengths))

    layer_out, pullback = jax.vjp(forward, params, embed_table.astype(jnp.float32))
    d_params, d_embed = pullback(grad_out.astype(jnp.float32))
    return (layer_out.astype(jnp.bfloat16), d_embed, d_params[0], d_params[1], d_params[2], d_params[3], d_params[4], d_params[5])
```

```python
import functools
import typing

import numpy as np
import jax
import jax.numpy as jnp
from jax import lax
from jax.experimental import pallas as pl
from jax.experimental.pallas import tpu as pltpu
from jax.sharding import PartitionSpec as P

MASK_ID = 32
LN_EPS = 1e-5
ROPE_BASE = 10000.0
TRAIN_RATIO = 0.15 * 0.8
NEG_BIG = -1e30
D = 480
INV_D = 1.0 / D
H = 20
HD = 24
HP = 32
QP = H * HP
NQKV = 2 * QP + D
F = 1920
S = 256
VP = 40
PIECES = 8
PV = D // PIECES
PR = 64
DX = PIECES * PR
FR = 256
FV = F // PIECES
SQRT_HALF = 0.7071067811865476
INV_SQRT_2PI = 0.3989422804014327
LANES = 128
HALF = 16
ROT = HD // 2
MIB = 2 ** 20
MESH = pl.DeviceIdType.MESH
QUARTERS = 4
GROUPS = H // QUARTERS

NN = (((1,), (0,)), ((), ()))
NT = (((1,), (1,)), ((), ()))


def dot(a, b, dims=NN):
    return lax.dot_general(a, b, dims, preferred_element_type=jnp.float32)


def eye(n):
    return (lax.broadcasted_iota(jnp.int32, (n, n), 0) == lax.broadcasted_iota(jnp.int32, (n, n), 1)).astype(jnp.float32).astype(jnp.bfloat16)


def fold(z):
    return z[:, :LANES] + z[:, LANES:]


def col_sum(z):
    return jnp.sum(z, axis=0, keepdims=True)


def chunks(total, width):
    return [slice(j, min(j + width, total)) for j in range(0, total, width)]


def zero(*refs):
    for ref in refs:
        ref[...] = jnp.zeros_like(ref)


def head(h, width=None):
    width = HP if width is None else width
    return slice(width * h, width * (h + 1))


def side_by_side(g, block):
    return jnp.concatenate([place(block(QUARTERS * g + slot), slot) for slot in range(QUARTERS)], axis=1)


def cols(ref):
    return [ref[:, j:j + 1] for j in range(6)]


def embed(tok, length, table_t):
    pos = lax.broadcasted_iota(jnp.int32, (1, S), 1)
    is_mask = tok == MASK_ID
    valid = pos < length
    n_mask = jnp.sum(is_mask.astype(jnp.float32), axis=1, keepdims=True)
    len_f = jnp.full((1, 1), length, jnp.int32).astype(jnp.float32)
    scale = (1.0 - TRAIN_RATIO) / (1.0 - n_mask / len_f)
    keep = jnp.where(is_mask | jnp.logical_not(valid), 0.0, scale)
    one_hot = (lax.broadcasted_iota(jnp.int32, (VP, S), 0) == tok).astype(jnp.float32).astype(jnp.bfloat16)
    return dot(table_t, one_hot) * keep, keep, one_hot, valid


def norm_stats(z):
    mean = col_sum(z) * INV_D
    cen = z - mean
    var = col_sum(cen * cen) * INV_D
    rstd = lax.rsqrt(var + LN_EPS)
    return cen * rstd, rstd


def norm_back(d_out, gain, xhat, rstd):
    d_hat = d_out * gain
    m1 = col_sum(d_hat) * INV_D
    m2 = col_sum(d_hat * xhat) * INV_D
    return rstd * (d_hat - m1 - xhat * m2)


def spread(z, src, dst):
    src[...] = z
    for j in range(PIECES):
        dst[PR * j:PR * j + PV, :] = src[PV * j:PV * (j + 1), :]
    return dst[...]


def pack(z, src, dst):
    src[...] = z
    for j in range(PIECES):
        dst[PV * j:PV * (j + 1), :] = src[PR * j:PR * j + PV, :]
    return dst[...]


def split3(z):
    parts = []
    for _ in range(3):
        parts.append(z.astype(jnp.bfloat16))
        z = z - parts[-1].astype(jnp.float32)
    return parts


def lane_sums(acc):
    ones = jnp.ones((8, LANES), jnp.bfloat16)
    hi, mid, lo = (dot(ones, part, NT)[:1] for part in split3(acc))
    return hi + (mid + lo)


def minus_rows(block, first, value):
    row = lax.broadcasted_iota(jnp.int32, block.shape, 0)
    for n, part in enumerate(split3(-value)):
        block = jnp.where(row == first + n, part.astype(jnp.float32), block)
    return block.astype(jnp.bfloat16)


def flip(w_ref, out, width):
    ident = eye(LANES)
    for sl in chunks(width, LANES):
        n = sl.stop - sl.start
        out[sl, :] = dot(ident[:n, :n], w_ref[:, sl], NT).astype(jnp.bfloat16)


def place(rows, slot):
    parts = []
    if slot:
        parts.append(jnp.zeros((HP * slot, S), rows.dtype))
    parts.append(rows)
    if slot < 3:
        parts.append(jnp.zeros((HP * (3 - slot), S), rows.dtype))
    return jnp.concatenate(parts, axis=0)


def rope_store(lin, out, base, ca, cb, sn):
    for h in range(H):
        lo, up = lin[HP * h:HP * h + HALF], lin[HP * h + HALF:HP * (h + 1)]
        out[0, base + HP * h:base + HP * h + HALF, :] = (lo * ca - up * sn).astype(jnp.bfloat16)
        out[0, base + HP * h + HALF:base + HP * (h + 1), :] = (up * cb + lo * sn).astype(jnp.bfloat16)


def attn_fwd_kernel(len_ref, tok_ref, table_ref, vec_ref, bias_ref, rope_ref, w_ref, wo_loc, wu_loc, wd_loc, g_loc, g_part,
                    q_out, k_out, krow_out, vrow_out, o_out, lse_out, wo_all, wu_all, wd_all, g_all,
                    wt, v_t, sp, sx, w_send, w_recv, g_send, g_recv, loc_sem):
    step = pl.program_id(0)
    last = pl.num_programs(0) - 1
    f, c = lax.axis_index('fsdp'), lax.axis_index('cp')
    pairs = [(wo_loc, wo_all), (wu_loc, wu_all), (wd_loc, wd_all)]
    g_puts, g_near = grad_puts(g_loc, g_all, pl.ds(EARLY, g_loc.shape[1] - EARLY), (g_send, g_recv), loc_sem.at[len(pairs)], c)
    w_puts = [copy_to(loc, full.at[f], (w_send.at[m], w_recv.at[m]), k, {'fsdp': f ^ k}) for m, (loc, full) in enumerate(pairs) for k in OWN_PUTS]
    w_fwds = [copy_to(full.at[f ^ k], full.at[f ^ k], (w_send.at[m], w_recv.at[m]), k + 1, {'fsdp': f ^ 1}) for m, (_, full) in enumerate(pairs) for k in FAR]
    local = [pltpu.make_async_copy(loc, full.at[f], loc_sem.at[m]) for m, (loc, full) in enumerate(pairs)]
    local.append(g_near)

    @pl.when(step == 0)
    def _():
        enter([{'fsdp': f ^ k} for k in OWN_PUTS] + [{'cp': (c + d) % QUARTERS} for d in range(1, QUARTERS)])
        for copy in w_puts + g_puts + local:
            copy.start()
        zero(sx)
        flip(w_ref, wt, NQKV)

    @pl.when(step == last - 1)
    def _():
        for m in range(len(pairs)):
            for n, k in enumerate(OWN_PUTS):
                if k in FAR:
                    w_puts[m * len(OWN_PUTS) + n].wait_recv()
        for copy in w_fwds:
            copy.start()

    e_t, _, _, valid = embed(tok_ref[0], len_ref[step], table_ref[...])
    xhat, _ = norm_stats(e_t)
    g1, c1, _, _, _, _ = cols(vec_ref)
    h_t = spread(xhat * g1 + c1, sp, sx).astype(jnp.bfloat16)
    mask_row = jnp.where(valid, 0.0, NEG_BIG)
    cos_q, cos_q2, sin_q, cos_k, sin_k, cos_k2 = (rope_ref[r] for r in range(6))
    cos_k2 = jnp.where(lax.broadcasted_iota(jnp.int32, (HALF, S), 0) == HALF - 1, mask_row, cos_k2)
    rope_store(dot(wt[:QP, :], h_t) + bias_ref[:QP, :], q_out, 0, cos_q, cos_q2, sin_q)
    rope_store(dot(wt[QP:2 * QP, :], h_t) + bias_ref[QP:2 * QP, :], k_out, 0, cos_k, cos_k2, sin_k)
    v_lin = dot(wt[2 * QP:, :], h_t) + bias_ref[2 * QP:, :]
    pad = (lax.broadcasted_iota(jnp.int32, (HP - HD, S), 0) < 3).astype(jnp.float32)
    for h in range(H):
        v_t[head(h), :] = jnp.concatenate([v_lin[head(h, HD)], pad], axis=0).astype(jnp.bfloat16)
    ident = eye(S)
    krow_out[0] = dot(ident, k_out[0], NT).astype(jnp.bfloat16)
    vrow_out[0] = dot(ident, v_t[...], NT).astype(jnp.bfloat16)
    def scores(g):
        return dot(krow_out[0, :, head(g, LANES)], side_by_side(g, lambda h: q_out[0, head(h), :]))

    def finish(h, top, tot, p):
        o_h = dot(v_t[head(h), :], p)
        o_out[0, head(h, HD), :] = o_h[:HD] / tot
        lse_out[0, h:h + 1, :] = top + jnp.log(tot)

    pending = None
    ahead = scores(0)
    for g in range(GROUPS):
        now = ahead
        if g + 1 < GROUPS:
            ahead = scores(g + 1)
        for slot in range(QUARTERS):
            sc = now[:, head(slot, S)]
            top = jnp.max(sc, axis=0, keepdims=True)
            p = jnp.exp(sc - top)
            if pending:
                finish(*pending)
            pending = (QUARTERS * g + slot, top, col_sum(p), p.astype(jnp.bfloat16))
    finish(*pending)

    @pl.when(step == last)
    def _():
        for n, copy in enumerate(w_puts):
            if OWN_PUTS[n % len(OWN_PUTS)] not in FAR:
                copy.wait_recv()
        for copy in w_fwds + g_puts:
            copy.wait_recv()
        for copy in local:
            copy.wait()
        for copy in w_puts + w_fwds + g_puts:
            copy.wait_send()


def ffn_kernel(len_ref, tok_ref, table_ref, vec_ref, bup_ref, o_ref, g_ref, wo_ref, wu_ref, wd_ref,
               dres_ref, dwd_ref, dwu_ref, sv_ref, out_all, wot, wut, wdt, gelu_s, dup_s, dbup_ref, dvec_ref, sp, sx, sy, obuf, o_send, o_recv, loc_sem):
    step = pl.program_id(0)
    n_step = pl.num_programs(0)
    c = lax.axis_index('cp')
    rows = S // QUARTERS

    def out_puts(i):
        slot = lax.rem(i, 2)
        part = lambda p: obuf.at[slot, pl.ds(pl.multiple_of(p * rows, rows), rows)]
        dst = out_all.at[c * n_step + i]
        far = [copy_to(part((c + d) % QUARTERS), dst, (o_send.at[i], o_recv.at[i]), d, {'cp': (c + d) % QUARTERS}) for d in NEAR_CP]
        return far, pltpu.make_async_copy(part(c), dst, loc_sem.at[i])

    @pl.when(step == 0)
    def _():
        enter([{'cp': (c + d) % QUARTERS} for d in range(1, QUARTERS)])
        zero(sx, dwd_ref, dwu_ref, dbup_ref, dvec_ref)
        flip(wo_ref, wot, D)
        flip(wd_ref, wdt, D)
        flip(wu_ref, wut, F)

    @pl.when(step >= 2)
    def _():
        far, near = out_puts(step - 2)
        near.wait()
        for copy in far:
            copy.wait_send()

    _, _, b_o, gain2, bias2, b_down = cols(vec_ref)
    e_t, _, _, _ = embed(tok_ref[0], len_ref[step], table_ref[...])
    o_x = spread(o_ref[0], sp, sx).astype(jnp.bfloat16)
    x1 = e_t + dot(wot[...], o_x) + b_o
    xhat, rstd = norm_stats(x1)
    n_t = spread(xhat * gain2 + bias2, sp, sx).astype(jnp.bfloat16)
    g_t32 = dot(eye(D), g_ref[...].reshape(S, D), NT)
    g_t = g_t32.astype(jnp.bfloat16)
    for sl in chunks(F, D):
        up = dot(wut[sl, :], n_t) + bup_ref[sl, :]
        d_gelu = dot(wd_ref[sl, :], g_t)
        cdf = 0.5 * (1.0 + lax.erf(up * SQRT_HALF))
        pdf = jnp.exp(up * up * -0.5) * INV_SQRT_2PI
        gelu_s[sl, :] = (up * cdf).astype(jnp.bfloat16)
        d_up = d_gelu * (cdf + up * pdf)
        dup_s[sl, :] = d_up.astype(jnp.bfloat16)
        dbup_ref[sl, :] += fold(d_up)
    out_t = (x1 + dot(wdt[...], gelu_s[...]) + b_down).astype(jnp.bfloat16)
    obuf[lax.rem(step, 2)] = dot(eye(S), out_t, NT).astype(jnp.bfloat16)
    for j in range(PIECES):
        dwd_ref[j, :FV, :] += dot(gelu_s[head(j, FV), :], g_t, NT)
    for sl in chunks(F, 3 * LANES):
        dwu_ref[:, sl] += dot(n_t, dup_s[sl, :], NT)
    d_n = pack(dot(wu_ref[...], dup_s[...]), sy, sp)
    d_res = g_t32 + norm_back(d_n, gain2, xhat, rstd)
    dres_ref[0] = d_res
    for r, z in enumerate((d_res, d_n * xhat, d_n, g_t32)):
        dvec_ref[r] += fold(z)
    far, near = out_puts(step)
    for copy in far + [near]:
        copy.start()

    @pl.when(step == n_step - 1)
    def _():
        for r in range(4):
            sv_ref[r:r + 1, :] = lane_sums(dbup_ref[head(r, D), :])
            sv_ref[r + 4:r + 5, :] = lane_sums(dvec_ref[r])
        for back in range(2):
            far, near = out_puts(step - back)
            near.wait()
            for copy in far:
                copy.wait_send()

        def drain(i, carry):
            for copy in out_puts(i)[0]:
                copy.wait_recv()
            return carry

        lax.fori_loop(0, n_step, drain, 0)


def attn_bwd_kernel(len_ref, tok_ref, table_ref, vec_ref, rope_ref, q_ref, k_ref, krow_ref, vrow_ref, o_ref, lse_ref, dres_ref, wo_ref, w_ref, sv_in, dwd_src, dwu_src,
                    dwo_ref, dw_ref, sv_ref, pd_ref, pu_ref, da_s, dq_s, dk_s, dlin_s, dcmp_s, dlinb_s, dbias_ref, dvec_ref, dtab_ref, sp, sx, sy, *comm):
    step = pl.program_id(0)
    f, c = lax.axis_index('fsdp'), lax.axis_index('cp')
    refs = list(comm)
    b_send, b_recv, loc_sem = refs[-3:]
    outs = [(dwd_src, pd_ref, sl) for sl in FFN_SPLITS[0]] + [(dwu_src, pu_ref, sl) for sl in FFN_SPLITS[1]]
    units = [Unit(src, sl, *refs[m:-3:len(outs)], b_send.at[m], b_recv.at[m], loc_sem.at[m]) for m, (src, _, sl) in enumerate(outs)]

    def advance(*todo):
        for m, stage in todo:
            settle(units[m], stage, f, c)
        for m, stage in todo:
            for copy in stage_copies(units[m], stage, f, c):
                copy.start()

    def comm_point(late):
        for i in range(H // 2):
            point = 2 * i + late
            todo = [(m, stage) for m in range(len(units)) for stage, at in enumerate(POINTS) if stage and at + 3 * m == point]
            if todo:
                pl.when(step == i)(functools.partial(advance, *todo))

    @pl.when(step == 0)
    def _():
        enter(reduce_peers(f, c))
        for u in units:
            for copy in loads(u, f):
                copy.start()
        advance(*((m, 0) for m in range(len(units))))
        zero(sx, dwo_ref, dw_ref, dtab_ref, dbias_ref, dvec_ref)

    comm_point(0)

    d_res = dres_ref[0]
    d_res_b = d_res.astype(jnp.bfloat16)
    dwo_ref[...] += dot(spread(o_ref[0], sp, sx).astype(jnp.bfloat16), d_res_b, NT)
    d_attn = pack(dot(wo_ref[...], d_res_b), sy, sp)
    prod = d_attn * o_ref[0]
    pad = jnp.zeros((HP - HD, S), jnp.float32)
    for h in range(H):
        delta = col_sum(prod[head(h, HD)])
        da_s[head(h), :] = jnp.concatenate([d_attn[head(h, HD)], minus_rows(pad, 0, delta).astype(jnp.float32)], axis=0).astype(jnp.bfloat16)
    def q_block(h):
        q_h = q_ref[0, head(h), :]
        q_up = minus_rows(q_h[HALF:].astype(jnp.float32), ROT, lse_ref[0, h:h + 1, :])
        return jnp.concatenate([q_h[:HALF], q_up], axis=0)

    def scores(g):
        lanes = head(g, LANES)
        return dot(krow_ref[0, :, lanes], side_by_side(g, q_block)), dot(vrow_ref[0, :, lanes], side_by_side(g, lambda h: da_s[head(h), :]))

    def finish(h, p, ds):
        rows = head(h)
        dq_s[rows, :] = dot(k_ref[0, rows, :], ds)
        dk_s[rows, :] = dot(q_ref[0, rows, :], ds, NT)
        d_v = dot(da_s[rows, :], p, NT)[:HD]
        dlin_s[2 * QP + HD * h:2 * QP + HD * (h + 1), :] = d_v
        dcmp_s[2 * D + HD * h:2 * D + HD * (h + 1), :] = d_v

    pending = None
    ahead = scores(0)
    for g in range(GROUPS):
        now = ahead
        if g + 1 < GROUPS:
            ahead = scores(g + 1)
        for slot in range(QUARTERS):
            sc, d_p = (z[:, head(slot, S)] for z in now)
            p = jnp.exp(sc)
            ds = (p * d_p).astype(jnp.bfloat16)
            if pending:
                finish(*pending)
            pending = (QUARTERS * g + slot, p.astype(jnp.bfloat16), ds)
    finish(*pending)
    comm_point(1)
    cos_q, _, sin_q, cos_k, sin_k = (rope_ref[r] for r in range(5))
    for m, (src, cs, sn) in enumerate(((dq_s, cos_q, sin_q), (dk_s, cos_k, sin_k))):
        for h in range(H):
            lo, up = src[HP * h:HP * h + HALF, :], src[HP * h + HALF:HP * (h + 1), :]
            for n, z in enumerate((lo * cs + up * sn, up * cs - lo * sn)):
                wide, slim = QP * m + HP * h + HALF * n, D * m + HD * h + ROT * n
                dlin_s[wide:wide + HALF, :] = z
                dcmp_s[slim:slim + ROT, :] = z[:ROT]
    d_cmp = dcmp_s[...]
    dbias_ref[...] += fold(d_cmp)
    dcmp_b = d_cmp.astype(jnp.bfloat16)
    dlinb_s[...] = dlin_s[...].astype(jnp.bfloat16)
    e_t, keep, one_hot, _ = embed(tok_ref[0], len_ref[step], table_ref[...])
    xhat, rstd = norm_stats(e_t)
    g1, c1, _, _, _, _ = cols(vec_ref)
    h_t = spread(xhat * g1 + c1, sp, sx).astype(jnp.bfloat16)
    for sl in chunks(3 * D, 3 * LANES):
        dw_ref[:, sl] += dot(h_t, dcmp_b[sl, :], NT)
    d_h = pack(dot(w_ref[...], dlinb_s[...]), sy, sp)
    d_e = (norm_back(d_h, g1, xhat, rstd) + d_res) * keep
    dtab_ref[...] += dot(one_hot, d_e.astype(jnp.bfloat16), NT)
    dvec_ref[0] += fold(d_h * xhat)
    dvec_ref[1] += fold(d_h)

    @pl.when(step == pl.num_programs(0) - 1)
    def _():
        zero(sv_ref)
        sv_ref[:8, :] = sv_in[...]
        for r in range(5):
            sums = dvec_ref[r] if r < 2 else dbias_ref[head(r - 2, D), :]
            sv_ref[8 + r:9 + r, :] = lane_sums(sums)
        sv_ref[HALF:, :] = dtab_ref[...]
        for u, (_, out, sl) in zip(units, outs):
            settle(u, STAGES, f, c)
            out[:, sl] = u.fin[:out.shape[0], :]
            for stage in range(STAGES):
                for copy in stage_copies(u, stage, f, c):
                    copy.wait_send()


def enter(peers):
    barrier = pltpu.get_barrier_semaphore()
    for peer in peers:
        pl.semaphore_signal(barrier, inc=1, device_id=peer, device_id_type=MESH)
    pl.semaphore_wait(barrier, len(peers))


def copy_to(src, dst, sems, k, peer):
    return pltpu.make_async_remote_copy(src_ref=src, dst_ref=dst, send_sem=sems[0].at[k], recv_sem=sems[1].at[k], device_id=peer, device_id_type=MESH)


OWN_PUTS = (2, 4, 6, 1)
EARLY = 3
NEAR_CP = (2, 1, 3)
FAR = (2, 4, 6)


def grad_puts(src, dst, seqs, sems, loc, c):
    far = [copy_to(src.at[(c + d) % QUARTERS, seqs], dst.at[c, seqs], sems, d, {'cp': (c + d) % QUARTERS}) for d in NEAR_CP]
    return far, pltpu.make_async_copy(src.at[c, seqs], dst.at[c, seqs], loc)


def gather_kernel(w_ref, small_ref, tok_ref, g_ref, w_out, small_out, tok_out, g_out, w_send, w_recv, s_send, s_recv, t_send, t_recv, g_send, g_recv, loc_sem):
    f, c = lax.axis_index('fsdp'), lax.axis_index('cp')
    enter([{'fsdp': f ^ k} for k in range(1, PIECES)] + [{'cp': (c + d) % QUARTERS} for d in range(1, QUARTERS)])
    w_sems = (w_send, w_recv)
    smalls = [copy_to(small_ref, small_out.at[f], (s_send, s_recv), k, {'fsdp': f ^ k}) for k in range(1, PIECES)]
    smalls += [copy_to(tok_ref.at[(c + d) % QUARTERS], tok_out.at[c], (t_send, t_recv), d, {'cp': (c + d) % QUARTERS}) for d in range(1, QUARTERS)]
    puts = [copy_to(w_ref, w_out.at[f], w_sems, k, {'fsdp': f ^ k}) for k in OWN_PUTS]
    fwds = [copy_to(w_out.at[f ^ k], w_out.at[f ^ k], w_sems, k + 1, {'fsdp': f ^ 1}) for k in FAR]
    local = [pltpu.make_async_copy(a, b, loc_sem.at[m]) for m, (a, b) in enumerate(((w_ref, w_out.at[f]), (tok_ref.at[c], tok_out.at[c]), (small_ref, small_out.at[f])))]
    far, near = grad_puts(g_ref, g_out, pl.ds(0, EARLY), (g_send, g_recv), loc_sem.at[len(local)], c)
    local.append(near)
    for copy in puts + smalls + local + far:
        copy.start()
    for put, fwd in zip(puts, fwds):
        put.wait_recv()
        fwd.start()
    for copy in puts[len(FAR):] + smalls + fwds + far:
        copy.wait_recv()
    for copy in local:
        copy.wait()
    for copy in puts + smalls + fwds + far:
        copy.wait_send()


class Unit(typing.NamedTuple):
    src: typing.Any
    lanes: slice
    acc: typing.Any
    core: typing.Any
    xy: typing.Any
    xy2: typing.Any
    z: typing.Any
    fin: typing.Any
    send: typing.Any
    recv: typing.Any
    loc: typing.Any


STAGES = 5
POINTS = (0, 1, 3, 4, 6)
FFN_SPLITS = ((slice(0, 2 * LANES), slice(2 * LANES, D)), (slice(0, 8 * LANES), slice(8 * LANES, F)))


def reduce_peers(f, c):
    return [{'fsdp': f ^ k} for k in (1, 2, 4)] + [{'cp': (c + d) % QUARTERS} for d in range(1, QUARTERS)]


def loads(u, f):
    return [pltpu.make_async_copy(u.src.at[f ^ (2 * q), :, u.lanes], u.acc.at[q], u.loc.at[q]) for q in range(QUARTERS)]


def stage_copies(u, stage, f, c):
    rows = u.fin.shape[0]
    half, quarter = rows // 2, rows // QUARTERS
    lo, hi = pl.ds(0, half), pl.ds(half, half)
    own = lambda p: pl.ds(pl.multiple_of(p * quarter, 8), quarter)
    core, xp, yp = ({'fsdp': f ^ k} for k in (1, 2, 4))
    ac = u.acc
    if stage == 0:
        plan = [(u.src.at[(f ^ 1) ^ (2 * q), :, u.lanes], u.core.at[q], core) for q in (3, 1, 2, 0)]
    elif stage == 1:
        plan = [(ac.at[3, lo], u.xy.at[1], xp), (ac.at[3, hi], u.xy.at[3], yp), (ac.at[1, lo], u.xy.at[0], xp), (ac.at[2, hi], u.xy.at[2], yp)]
    elif stage == 2:
        plan = [(ac.at[2, lo], u.xy2.at[0], yp), (ac.at[1, hi], u.xy2.at[1], xp)]
    elif stage == 3:
        plan = [(ac.at[0, own((c + d) % QUARTERS)], u.z.at[d - 1], {'cp': (c + d) % QUARTERS}) for d in NEAR_CP]
    else:
        plan = [(u.fin.at[own(c)], u.fin.at[own(c)], {'cp': (c + d) % QUARTERS}) for d in NEAR_CP]
    return [copy_to(a, b, (u.send, u.recv), QUARTERS * stage + n, peer) for n, (a, b, peer) in enumerate(plan)]


def settle(u, stage, f, c):
    if not stage:
        return
    for copy in stage_copies(u, stage - 1, f, c):
        copy.wait_recv()
    rows = u.fin.shape[0]
    half, quarter = rows // 2, rows // QUARTERS
    lo, hi = slice(0, half), slice(half, rows)
    if stage == 1:
        for copy in loads(u, f):
            copy.wait()
        u.acc[...] += u.core[...]
    elif stage == 2:
        for q, part, n in ((2, lo, 1), (1, hi, 3), (0, lo, 0), (0, hi, 2)):
            u.acc[q, part] += u.xy[n]
    elif stage == 3:
        u.acc[0, lo] += u.xy2[0]
        u.acc[0, hi] += u.xy2[1]
    elif stage == QUARTERS:
        mine = pl.ds(pl.multiple_of(c * quarter, 8), quarter)
        u.fin[mine] = (u.acc[0, mine] + u.z[0]) + (u.z[1] + u.z[2])


def reduce_kernel(dw_src, dwo_src, small, d_qkv, d_out, small_out, buf, r_small, *refs):
    n_unit = len(SPLITS) + 1
    refs = list(refs)
    b_send, b_recv, m_send, m_recv, loc_sem = refs[-5:]
    refs = refs[:-5]
    f, c = lax.axis_index('fsdp'), lax.axis_index('cp')
    enter(reduce_peers(f, c))
    outs = [(dwo_src, d_out, slice(0, D))] + [(dw_src, d_qkv, sl) for sl in SPLITS]
    units = [Unit(src, sl, *refs[m::n_unit], b_send.at[m], b_recv.at[m], loc_sem.at[m]) for m, (src, _, sl) in enumerate(outs)]
    steps = [{'fsdp': f ^ k} for k in (1, 2, 4)] + [{'cp': c ^ 1}, {'cp': c ^ 2}]
    small_puts = [copy_to(buf.at[t], r_small.at[t], (m_send, m_recv), t, peer) for t, peer in enumerate(steps)]
    for u in units:
        for copy in loads(u, f):
            copy.start()
    for t in range(n_unit + STAGES):
        todo = [(m, t - m) for m in range(n_unit) if 0 <= t - m <= STAGES]
        for m, stage in todo:
            settle(units[m], stage, f, c)
            if stage == STAGES:
                _, out, sl = outs[m]
                out[:, sl] = units[m].fin[:PV, :]
        if t <= STAGES:
            if t:
                small_puts[t - 1].wait_recv()
            value = buf[t - 1] + r_small[t - 1] if t else small[...]
            if t < STAGES:
                buf[t] = value
            else:
                small_out[...] = value
        for m, stage in todo:
            if stage < STAGES:
                for copy in stage_copies(units[m], stage, f, c):
                    copy.start()
        if t < STAGES:
            small_puts[t].start()
    for copy in small_puts:
        copy.wait_send()
    for u in units:
        for stage in range(STAGES):
            for copy in stage_copies(u, stage, f, c):
                copy.wait_send()


def rope_tables():
    inv_freq = (1.0 / (ROPE_BASE ** (np.arange(0, HD, 2, dtype=np.float32) / np.float32(HD)))).astype(np.float32)
    angles = inv_freq[:, None] * np.arange(S, dtype=np.float32)[None, :]
    cos, sin = np.zeros((16, S), np.float32), np.zeros((16, S), np.float32)
    cos[:12], sin[:12] = np.cos(angles), np.sin(angles)
    scale = np.float32(HD ** -0.5)
    cos_q2 = cos * scale
    cos_q2[15] = 1.0
    cos_k2 = cos.copy()
    cos_k2[ROT:] = 1.0
    return np.stack([cos * scale, cos_q2, sin * scale, cos, sin, cos_k2])


def pad_heads(z):
    lead = z.shape[:-2]
    z = z.reshape(lead + (H, 2, HD // 2))
    z = jnp.pad(z, [(0, 0)] * len(lead) + [(0, 0), (0, 0), (0, 4)])
    return z.reshape(lead + (QP,))


def const(shape):
    return pl.BlockSpec(shape, lambda i, *_: (0,) * len(shape))


def per_seq(shape):
    return pl.BlockSpec((1,) + shape, lambda i, *_: (i,) + (0,) * len(shape))


def anys(n):
    return [pl.BlockSpec(memory_space=pl.ANY)] * n


def dma(*shape):
    return pltpu.SemaphoreType.DMA(shape)


def gather_all(w_loc, small, tok4, grad4):
    return pl.pallas_call(
        gather_kernel,
        in_specs=anys(4),
        out_specs=anys(4),
        out_shape=[b16(PIECES, *w_loc.shape), f32(PIECES, *small.shape), jax.ShapeDtypeStruct(tok4.shape, tok4.dtype), b16(*grad4.shape)],
        scratch_shapes=[dma(PIECES)] * 4 + [dma(QUARTERS)] * 5,
        compiler_params=pltpu.CompilerParams(collective_id=1, has_side_effects=True),
        name="gather_all",
    )(w_loc, small, tok4, grad4)


def unit_scratch(parts):
    v = lambda *shape: pltpu.VMEM(shape, jnp.float32)
    out = []
    for lead, div in ((4, 1), (4, 1), (4, 2), (2, 2), (3, 4)):
        out += [v(lead, r // div, n) for r, n in parts]
    return out + [v(r, n) for r, n in parts]


SPLITS = (slice(0, 6 * LANES), slice(6 * LANES, 3 * D))


def reduce_all(dw, dwo, small):
    vmem = pl.BlockSpec(memory_space=pltpu.VMEM)
    parts = [(PR, D)] + [(PR, sl.stop - sl.start) for sl in SPLITS]
    n = len(parts)
    scratch = [pltpu.VMEM((STAGES,) + small.shape, jnp.float32)] * 2 + unit_scratch(parts)
    scratch += [dma(n, QUARTERS * STAGES)] * 2 + [dma(STAGES)] * 2 + [dma(n, QUARTERS)]
    return pl.pallas_call(
        reduce_kernel,
        in_specs=anys(2) + [vmem],
        out_specs=[vmem] * 3,
        out_shape=[f32(PV, 3 * D), f32(PV, D), f32(*small.shape)],
        scratch_shapes=scratch,
        compiler_params=pltpu.CompilerParams(collective_id=2, has_side_effects=True, vmem_limit_bytes=58 * MIB),
        name="reduce_all",
    )(dw, dwo, small)


def call(kernel, cid, n, in_specs, out_specs, out_shape, scratch, flops, name, aliases={}):
    return pl.pallas_call(
        kernel,
        grid_spec=pltpu.PrefetchScalarGridSpec(num_scalar_prefetch=1, grid=(n,), in_specs=in_specs, out_specs=out_specs, scratch_shapes=scratch),
        out_shape=out_shape,
        compiler_params=pltpu.CompilerParams(dimension_semantics=("arbitrary",), vmem_limit_bytes=58 * MIB, collective_id=cid, has_side_effects=True),
        input_output_aliases=aliases,
        cost_estimate=pl.CostEstimate(flops=flops, bytes_accessed=20 * MIB, transcendentals=0),
        name=name,
    )


def f32(*shape):
    return jax.ShapeDtypeStruct(shape, jnp.float32)


def b16(*shape):
    return jax.ShapeDtypeStruct(shape, jnp.bfloat16)


def sv(*shape):
    return pltpu.VMEM(shape, jnp.float32)


def bv(*shape):
    return pltpu.VMEM(shape, jnp.bfloat16)


def solution(mesh):
    n_cp, n_fsdp = mesh.shape['cp'], mesh.shape['fsdp']

    def local_step(tokens, lengths, embed_table, layer_vecs, w_qkv, w_out, w_up, b_up, w_down, grad_out):
        n_seq, seq_loc = tokens.shape
        n = n_seq // n_cp
        cp_index, f_index = lax.axis_index('cp'), lax.axis_index('fsdp')
        rows_pad = lambda w: jnp.pad(w, ((0, PR - PV), (0, 0)))
        w_loc = jnp.concatenate([pad_heads(w_qkv[:, 0]), pad_heads(w_qkv[:, 1]), w_qkv[:, 2].reshape(PV, D)], axis=1)
        small = jnp.pad(jnp.concatenate([layer_vecs.reshape(-1), b_up]), (0, PIECES * LANES - 9 * PV - FV)).reshape(PIECES, LANES)
        grad4 = grad_out.reshape(n_cp, n, seq_loc, D)
        w_full, small, tok, grads = gather_all(rows_pad(w_loc), small, tokens.reshape(n_cp, n, seq_loc), grad4)
        w_full = w_full.reshape(DX, NQKV)
        small = small.reshape(n_fsdp, PIECES * LANES)
        vecs = small[:, :9 * PV].reshape(n_fsdp, 9, PV).transpose(1, 0, 2).reshape(9, D)
        bup = small[:, 9 * PV:9 * PV + FV].reshape(F, 1)
        tok = tok.transpose(1, 0, 2).reshape(n, 1, S)
        lens = lax.dynamic_slice(lengths, (cp_index * n,), (n,))
        table_t = jnp.pad(embed_table, ((0, VP - embed_table.shape[0]), (0, 0))).T
        vec_cols = jnp.concatenate([vecs[:2], vecs[5:], jnp.zeros((2, D), jnp.float32)], axis=0).T
        slot = np.arange(QP) % HP
        pad_one = jnp.asarray(np.stack([slot == HP - 1, slot >= HALF + ROT]).astype(np.float32))
        bias = jnp.concatenate([(pad_heads(vecs[2:4].reshape(2, H, HD)) + pad_one).reshape(2 * QP), vecs[4]])[:, None]
        rope = jnp.asarray(rope_tables())

        shared = [per_seq((1, S)), const((D, VP)), const((D, 8))]
        rope_spec = const(rope.shape)
        acts = [((QP, S), b16), ((QP, S), b16), ((S, QP), b16), ((S, QP), b16), ((D, S), f32), ((24, S), f32)]
        act_specs = [per_seq(shape) for shape, _ in acts]
        fwd = call(
            attn_fwd_kernel, 3, n,
            shared + [const((NQKV, 1)), rope_spec, const((DX, NQKV))] + anys(5),
            act_specs + anys(4),
            [kind(n, *shape) for shape, kind in acts] + [b16(PIECES, PR, D), b16(PIECES, PR, F), b16(PIECES, FV, D), b16(n_cp, n, seq_loc, D)],
            [bv(NQKV, DX), bv(QP, S), sv(D, S), sv(DX, S)] + [dma(3, PIECES)] * 2 + [dma(QUARTERS)] * 3,
            int(2e10), "attn_fwd", {11: 9})(lens, tok, table_t, vec_cols, bias, rope, w_full, rows_pad(w_out), rows_pad(w_up), w_down, grad4, grads)
        acts, (out_w, up_w, down_w, grads) = fwd[:6], fwd[6:]
        out_w, up_w, down_w = out_w.reshape(DX, D), up_w.reshape(DX, F), down_w.reshape(F, D)
        d_res, dwd, dwu, sv2, layer_out = call(
            ffn_kernel, 4, n,
            shared + [const((F, 1)), per_seq((D, S)), pl.BlockSpec((n_cp, 1, seq_loc, D), lambda i, *_: (0, i, 0, 0)), const((DX, D)), const((DX, F)), const((F, D))],
            [per_seq((D, S)), const((PIECES, FR, D)), const((DX, F)), const((8, D))] + anys(1),
            [f32(n, D, S), f32(PIECES, FR, D), f32(DX, F), f32(8, D), b16(n_seq, seq_loc, D)],
            [bv(D, DX), bv(F, DX), bv(D, F), bv(F, S), bv(F, S), sv(F, LANES), sv(4, D, LANES), sv(D, S), sv(DX, S), sv(DX, S), bv(2, S, D)]
            + [dma(n, QUARTERS)] * 2 + [dma(n)],
            int(4e10), "ffn")(lens, tok, table_t, vec_cols, bup, acts[4], grads, out_w, up_w, down_w)
        ffn_parts = [(r, sl.stop - sl.start) for r, splits in zip((FR, PR), FFN_SPLITS) for sl in splits]
        cut = lambda z: z.reshape(PIECES, PR, z.shape[1])
        dwo, dw, smalls, d_down_w, d_up_w = call(
            attn_bwd_kernel, 5, n,
            shared + [rope_spec] + act_specs + [per_seq((D, S)), const((DX, D)), const((DX, NQKV)), const((8, D))] + anys(2),
            [const((DX, D)), const((DX, 3 * D)), const((HALF + VP, D)), const((FV, D)), const((PV, F))],
            [f32(DX, D), f32(DX, 3 * D), f32(HALF + VP, D), f32(FV, D), f32(PV, F)],
            [bv(QP, S), sv(QP, S), sv(QP, S), sv(NQKV, S), sv(3 * D, S), bv(NQKV, S), sv(3 * D, LANES), sv(2, D, LANES), sv(VP, D), sv(D, S), sv(DX, S), sv(DX, S)]
            + unit_scratch(ffn_parts) + [dma(4, QUARTERS * STAGES)] * 2 + [dma(4, QUARTERS)],
            int(5e10), "attn_bwd")(lens, tok, table_t, vec_cols, rope, *acts, d_res, out_w, w_full, sv2, dwd, cut(dwu))
        d_qkv, d_out_w, smalls = reduce_all(cut(dw), cut(dwo), smalls)
        d_qkv = d_qkv.reshape((PV,) + w_qkv.shape[1:])
        all_vecs = jnp.concatenate([smalls[8:13], smalls[4:8]], axis=0)
        d_vecs = lax.dynamic_slice(all_vecs, (0, f_index * PV), (9, PV))
        d_bup = lax.dynamic_slice(smalls[:4].reshape(F), (f_index * FV,), (FV,))
        return layer_out, smalls[HALF:HALF + embed_table.shape[0]], d_vecs, d_qkv, d_out_w, d_up_w, d_bup, d_down_w

    rows = P('fsdp', None)
    in_specs = (P('fsdp', 'cp'), P('fsdp'), P(), P(None, 'fsdp'), P('fsdp', None, None, None), rows, rows, P('fsdp'), rows, P('fsdp', 'cp', None))
    out_specs = (P('fsdp', 'cp', None), P(), P(None, 'fsdp'), P('fsdp', None, None, None), rows, rows, P('fsdp'), rows)
    return jax.shard_map(local_step, mesh=mesh, in_specs=in_specs, out_specs=out_specs, check_vma=False)
```

```python
import functools
import typing

import numpy as np
import jax
import jax.numpy as jnp
from jax import lax
from jax.experimental import pallas as pl
from jax.experimental.pallas import tpu as pltpu
from jax.sharding import PartitionSpec as P

MASK_ID = 32
LN_EPS = 1e-5
ROPE_BASE = 10000.0
TRAIN_RATIO = 0.15 * 0.8
NEG_BIG = -1e30
D = 480
INV_D = 1.0 / D
H = 20
HD = 24
HP = 32
QP = H * HP
NQKV = 2 * QP + D
F = 1920
S = 256
VP = 40
PIECES = 8
PV = D // PIECES
PR = 64
DX = PIECES * PR
FR = 256
FV = F // PIECES
SQRT_HALF = 0.7071067811865476
INV_SQRT_2PI = 0.3989422804014327
LANES = 128
HALF = 16
ROT = HD // 2
MIB = 2 ** 20
MESH = pl.DeviceIdType.MESH
QUARTERS = 4
GROUPS = H // QUARTERS

NN = (((1,), (0,)), ((), ()))
NT = (((1,), (1,)), ((), ()))


def dot(a, b, dims=NN):
    return lax.dot_general(a, b, dims, preferred_element_type=jnp.float32)


def eye(n):
    return (lax.broadcasted_iota(jnp.int32, (n, n), 0) == lax.broadcasted_iota(jnp.int32, (n, n), 1)).astype(jnp.float32).astype(jnp.bfloat16)


def fold(z):
    return z[:, :LANES] + z[:, LANES:]


def col_sum(z):
    return jnp.sum(z, axis=0, keepdims=True)


def chunks(total, width):
    return [slice(j, min(j + width, total)) for j in range(0, total, width)]


def zero(*refs):
    for ref in refs:
        ref[...] = jnp.zeros_like(ref)


def head(h, width=None):
    width = HP if width is None else width
    return slice(width * h, width * (h + 1))


def side_by_side(g, block):
    return jnp.concatenate([place(block(QUARTERS * g + slot), slot) for slot in range(QUARTERS)], axis=1)


def cols(ref):
    return [ref[:, j:j + 1] for j in range(6)]


def embed(tok, length, table_t):
    pos = lax.broadcasted_iota(jnp.int32, (1, S), 1)
    is_mask = tok == MASK_ID
    valid = pos < length
    n_mask = jnp.sum(is_mask.astype(jnp.float32), axis=1, keepdims=True)
    len_f = jnp.full((1, 1), length, jnp.int32).astype(jnp.float32)
    scale = (1.0 - TRAIN_RATIO) / (1.0 - n_mask / len_f)
    keep = jnp.where(is_mask | jnp.logical_not(valid), 0.0, scale)
    one_hot = (lax.broadcasted_iota(jnp.int32, (VP, S), 0) == tok).astype(jnp.float32).astype(jnp.bfloat16)
    return dot(table_t, one_hot) * keep, keep, one_hot, valid


def norm_stats(z):
    mean = col_sum(z) * INV_D
    cen = z - mean
    var = col_sum(cen * cen) * INV_D
    rstd = lax.rsqrt(var + LN_EPS)
    return cen * rstd, rstd


def norm_back(d_out, gain, xhat, rstd):
    d_hat = d_out * gain
    m1 = col_sum(d_hat) * INV_D
    m2 = col_sum(d_hat * xhat) * INV_D
    return rstd * (d_hat - m1 - xhat * m2)


def spread(z, src, dst):
    src[...] = z
    for j in range(PIECES):
        dst[PR * j:PR * j + PV, :] = src[PV * j:PV * (j + 1), :]
    return dst[...]


def pack(z, src, dst):
    src[...] = z
    for j in range(PIECES):
        dst[PV * j:PV * (j + 1), :] = src[PR * j:PR * j + PV, :]
    return dst[...]


def split3(z):
    parts = []
    for _ in range(3):
        parts.append(z.astype(jnp.bfloat16))
        z = z - parts[-1].astype(jnp.float32)
    return parts


def lane_sums(acc):
    ones = jnp.ones((8, LANES), jnp.bfloat16)
    hi, mid, lo = (dot(ones, part, NT)[:1] for part in split3(acc))
    return hi + (mid + lo)


def minus_rows(block, first, value):
    row = lax.broadcasted_iota(jnp.int32, block.shape, 0)
    for n, part in enumerate(split3(-value)):
        block = jnp.where(row == first + n, part.astype(jnp.float32), block)
    return block.astype(jnp.bfloat16)


def flip(w_ref, out, width):
    ident = eye(LANES)
    for sl in chunks(width, LANES):
        n = sl.stop - sl.start
        out[sl, :] = dot(ident[:n, :n], w_ref[:, sl], NT).astype(jnp.bfloat16)


def place(rows, slot):
    parts = []
    if slot:
        parts.append(jnp.zeros((HP * slot, S), rows.dtype))
    parts.append(rows)
    if slot < 3:
        parts.append(jnp.zeros((HP * (3 - slot), S), rows.dtype))
    return jnp.concatenate(parts, axis=0)


def rope_store(lin, out, base, ca, cb, sn):
    for h in range(H):
        lo, up = lin[HP * h:HP * h + HALF], lin[HP * h + HALF:HP * (h + 1)]
        out[0, base + HP * h:base + HP * h + HALF, :] = (lo * ca - up * sn).astype(jnp.bfloat16)
        out[0, base + HP * h + HALF:base + HP * (h + 1), :] = (up * cb + lo * sn).astype(jnp.bfloat16)


def attn_fwd_kernel(len_ref, tok_ref, table_ref, vec_ref, bias_ref, rope_ref, w_ref, wo_loc, wu_loc, wd_loc, g_loc, g_part,
                    q_out, k_out, krow_out, vrow_out, o_out, lse_out, wo_all, wu_all, wd_all, g_all,
                    wt, v_t, sp, sx, w_send, w_recv, g_send, g_recv, loc_sem):
    step = pl.program_id(0)
    last = pl.num_programs(0) - 1
    f, c = lax.axis_index('fsdp'), lax.axis_index('cp')
    pairs = [(wo_loc, wo_all), (wu_loc, wu_all), (wd_loc, wd_all)]
    g_puts, g_near = grad_puts(g_loc, g_all, pl.ds(EARLY, g_loc.shape[1] - EARLY), (g_send, g_recv), loc_sem.at[len(pairs)], c)
    w_puts = [copy_to(loc, full.at[f], (w_send.at[m], w_recv.at[m]), k, {'fsdp': f ^ k}) for m, (loc, full) in enumerate(pairs) for k in OWN_PUTS]
    w_fwds = [copy_to(full.at[f ^ k], full.at[f ^ k], (w_send.at[m], w_recv.at[m]), k + 1, {'fsdp': f ^ 1}) for m, (_, full) in enumerate(pairs) for k in FAR]
    local = [pltpu.make_async_copy(loc, full.at[f], loc_sem.at[m]) for m, (loc, full) in enumerate(pairs)]
    local.append(g_near)

    @pl.when(step == 0)
    def _():
        enter([{'fsdp': f ^ k} for k in OWN_PUTS] + [{'cp': (c + d) % QUARTERS} for d in range(1, QUARTERS)])
        for copy in w_puts + g_puts + local:
            copy.start()
        zero(sx)
        flip(w_ref, wt, NQKV)

    @pl.when(step == last - 1)
    def _():
        for m in range(len(pairs)):
            for n, k in enumerate(OWN_PUTS):
                if k in FAR:
                    w_puts[m * len(OWN_PUTS) + n].wait_recv()
        for copy in w_fwds:
            copy.start()

    e_t, _, _, valid = embed(tok_ref[0], len_ref[step], table_ref[...])
    xhat, _ = norm_stats(e_t)
    g1, c1, _, _, _, _ = cols(vec_ref)
    h_t = spread(xhat * g1 + c1, sp, sx).astype(jnp.bfloat16)
    mask_row = jnp.where(valid, 0.0, NEG_BIG)
    cos_q, cos_q2, sin_q, cos_k, sin_k, cos_k2 = (rope_ref[r] for r in range(6))
    cos_k2 = jnp.where(lax.broadcasted_iota(jnp.int32, (HALF, S), 0) == HALF - 1, mask_row, cos_k2)
    rope_store(dot(wt[:QP, :], h_t) + bias_ref[:QP, :], q_out, 0, cos_q, cos_q2, sin_q)
    rope_store(dot(wt[QP:2 * QP, :], h_t) + bias_ref[QP:2 * QP, :], k_out, 0, cos_k, cos_k2, sin_k)
    v_lin = dot(wt[2 * QP:, :], h_t) + bias_ref[2 * QP:, :]
    pad = (lax.broadcasted_iota(jnp.int32, (HP - HD, S), 0) < 3).astype(jnp.float32)
    for h in range(H):
        v_t[head(h), :] = jnp.concatenate([v_lin[head(h, HD)], pad], axis=0).astype(jnp.bfloat16)
    ident = eye(S)
    krow_out[0] = dot(ident, k_out[0], NT).astype(jnp.bfloat16)
    vrow_out[0] = dot(ident, v_t[...], NT).astype(jnp.bfloat16)
    def scores(g):
        return dot(krow_out[0, :, head(g, LANES)], side_by_side(g, lambda h: q_out[0, head(h), :]))

    def finish(h, top, tot, p):
        o_h = dot(v_t[head(h), :], p)
        o_out[0, head(h, HD), :] = o_h[:HD] / tot
        lse_out[0, h:h + 1, :] = top + jnp.log(tot)

    pending = None
    ahead = scores(0)
    for g in range(GROUPS):
        now = ahead
        if g + 1 < GROUPS:
            ahead = scores(g + 1)
        for slot in range(QUARTERS):
            sc = now[:, head(slot, S)]
            top = jnp.max(sc, axis=0, keepdims=True)
            p = jnp.exp(sc - top)
            if pending:
                finish(*pending)
            pending = (QUARTERS * g + slot, top, col_sum(p), p.astype(jnp.bfloat16))
    finish(*pending)

    @pl.when(step == last)
    def _():
        for n, copy in enumerate(w_puts):
            if OWN_PUTS[n % len(OWN_PUTS)] not in FAR:
                copy.wait_recv()
        for copy in w_fwds + g_puts:
            copy.wait_recv()
        for copy in local:
            copy.wait()
        for copy in w_puts + w_fwds + g_puts:
            copy.wait_send()


def ffn_kernel(len_ref, tok_ref, table_ref, vec_ref, bup_ref, o_ref, g_ref, wo_ref, wu_ref, wd_ref,
               dres_ref, dwd_ref, dwu_ref, sv_ref, out_all, wot, wut, wdt, gelu_s, dup_s, dbup_ref, dvec_ref, sp, sx, sy, obuf, o_send, o_recv, loc_sem):
    step = pl.program_id(0)
    n_step = pl.num_programs(0)
    c = lax.axis_index('cp')
    rows = S // QUARTERS

    def out_puts(i):
        slot = lax.rem(i, 2)
        part = lambda p: obuf.at[slot, pl.ds(pl.multiple_of(p * rows, rows), rows)]
        dst = out_all.at[c * n_step + i]
        far = [copy_to(part((c + d) % QUARTERS), dst, (o_send.at[i], o_recv.at[i]), d, {'cp': (c + d) % QUARTERS}) for d in NEAR_CP]
        return far, pltpu.make_async_copy(part(c), dst, loc_sem.at[i])

    @pl.when(step == 0)
    def _():
        enter([{'cp': (c + d) % QUARTERS} for d in range(1, QUARTERS)])
        zero(sx, dwd_ref, dwu_ref, dbup_ref, dvec_ref)
        flip(wo_ref, wot, D)
        flip(wd_ref, wdt, D)
        flip(wu_ref, wut, F)

    @pl.when(step >= 2)
    def _():
        far, near = out_puts(step - 2)
        near.wait()
        for copy in far:
            copy.wait_send()

    _, _, b_o, gain2, bias2, b_down = cols(vec_ref)
    e_t, _, _, _ = embed(tok_ref[0], len_ref[step], table_ref[...])
    o_x = spread(o_ref[0], sp, sx).astype(jnp.bfloat16)
    x1 = e_t + dot(wot[...], o_x) + b_o
    xhat, rstd = norm_stats(x1)
    n_t = spread(xhat * gain2 + bias2, sp, sx).astype(jnp.bfloat16)
    g_t32 = dot(eye(D), g_ref[...].reshape(S, D), NT)
    g_t = g_t32.astype(jnp.bfloat16)
    def products(sl):
        return dot(wut[sl, :], n_t), dot(wd_ref[sl, :], g_t)

    parts = chunks(F, D)
    ahead = products(parts[0])
    for n, sl in enumerate(parts):
        up, d_gelu = ahead
        if n + 1 < len(parts):
            ahead = products(parts[n + 1])
        up = up + bup_ref[sl, :]
        cdf = 0.5 * (1.0 + lax.erf(up * SQRT_HALF))
        pdf = jnp.exp(up * up * -0.5) * INV_SQRT_2PI
        gelu_s[sl, :] = (up * cdf).astype(jnp.bfloat16)
        d_up = d_gelu * (cdf + up * pdf)
        dup_s[sl, :] = d_up.astype(jnp.bfloat16)
        dbup_ref[sl, :] += fold(d_up)
    out_t = (x1 + dot(wdt[...], gelu_s[...]) + b_down).astype(jnp.bfloat16)
    obuf[lax.rem(step, 2)] = dot(eye(S), out_t, NT).astype(jnp.bfloat16)
    d_down = dot(gelu_s[...], g_t, NT)
    for j in range(PIECES):
        dwd_ref[j, :FV, :] += d_down[head(j, FV)]
    far, near = out_puts(step)
    for copy in far + [near]:
        copy.start()
    for sl in chunks(F, 4 * LANES):
        dwu_ref[:, sl] += dot(n_t, dup_s[sl, :], NT)
    d_n = pack(dot(wu_ref[...], dup_s[...]), sy, sp)
    d_res = g_t32 + norm_back(d_n, gain2, xhat, rstd)
    dres_ref[0] = d_res
    for r, z in enumerate((d_res, d_n * xhat, d_n, g_t32)):
        dvec_ref[r] += fold(z)

    @pl.when(step == n_step - 1)
    def _():
        for r in range(4):
            sv_ref[r:r + 1, :] = lane_sums(dbup_ref[head(r, D), :])
            sv_ref[r + 4:r + 5, :] = lane_sums(dvec_ref[r])
        for back in range(2):
            far, near = out_puts(step - back)
            near.wait()
            for copy in far:
                copy.wait_send()

        def drain(i, carry):
            for copy in out_puts(i)[0]:
                copy.wait_recv()
            return carry

        lax.fori_loop(0, n_step, drain, 0)


def attn_bwd_kernel(len_ref, tok_ref, table_ref, vec_ref, rope_ref, q_ref, k_ref, krow_ref, vrow_ref, o_ref, lse_ref, dres_ref, wo_ref, w_ref, sv_in, dwd_src, dwu_src,
                    dwo_ref, dw_ref, sv_ref, pd_ref, pu_ref, da_s, dq_s, dk_s, dlin_s, dcmp_s, dlinb_s, dbias_ref, dvec_ref, dtab_ref, sp, sx, sy, *comm):
    step = pl.program_id(0)
    f, c = lax.axis_index('fsdp'), lax.axis_index('cp')
    refs = list(comm)
    b_send, b_recv, loc_sem = refs[-3:]
    outs = [(dwd_src, pd_ref, sl) for sl in FFN_SPLITS[0]] + [(dwu_src, pu_ref, sl) for sl in FFN_SPLITS[1]]
    units = [Unit(src, sl, *refs[m:-3:len(outs)], b_send.at[m], b_recv.at[m], loc_sem.at[m]) for m, (src, _, sl) in enumerate(outs)]

    def advance(*todo):
        for m, stage in todo:
            settle(units[m], stage, f, c)
        for m, stage in todo:
            for copy in stage_copies(units[m], stage, f, c):
                copy.start()

    def comm_point(late):
        for i in range(H // 2):
            point = 2 * i + late
            todo = [(m, stage) for m in range(len(units)) for stage, at in enumerate(POINTS) if stage and at + 3 * m == point]
            if todo:
                pl.when(step == i)(functools.partial(advance, *todo))

    @pl.when(step == 0)
    def _():
        enter(reduce_peers(f, c))
        for u in units:
            for copy in loads(u, f):
                copy.start()
        advance(*((m, 0) for m in range(len(units))))
        zero(sx, dwo_ref, dw_ref, dtab_ref, dbias_ref, dvec_ref)

    comm_point(0)

    d_res = dres_ref[0]
    d_res_b = d_res.astype(jnp.bfloat16)
    dwo_ref[...] += dot(spread(o_ref[0], sp, sx).astype(jnp.bfloat16), d_res_b, NT)
    d_attn = pack(dot(wo_ref[...], d_res_b), sy, sp)
    prod = d_attn * o_ref[0]
    pad = jnp.zeros((HP - HD, S), jnp.float32)
    for h in range(H):
        delta = col_sum(prod[head(h, HD)])
        da_s[head(h), :] = jnp.concatenate([d_attn[head(h, HD)], minus_rows(pad, 0, delta).astype(jnp.float32)], axis=0).astype(jnp.bfloat16)
    def q_block(h):
        q_h = q_ref[0, head(h), :]
        q_up = minus_rows(q_h[HALF:].astype(jnp.float32), ROT, lse_ref[0, h:h + 1, :])
        return jnp.concatenate([q_h[:HALF], q_up], axis=0)

    def scores(g):
        lanes = head(g, LANES)
        return dot(krow_ref[0, :, lanes], side_by_side(g, q_block)), dot(vrow_ref[0, :, lanes], side_by_side(g, lambda h: da_s[head(h), :]))

    def finish(h, p, ds):
        rows = head(h)
        dq_s[rows, :] = dot(k_ref[0, rows, :], ds)
        dk_s[rows, :] = dot(q_ref[0, rows, :], ds, NT)
        d_v = dot(da_s[rows, :], p, NT)[:HD]
        dlin_s[2 * QP + HD * h:2 * QP + HD * (h + 1), :] = d_v
        dcmp_s[2 * D + HD * h:2 * D + HD * (h + 1), :] = d_v

    pending = None
    ahead = scores(0)
    for g in range(GROUPS):
        now = ahead
        if g + 1 < GROUPS:
            ahead = scores(g + 1)
        for slot in range(QUARTERS):
            sc, d_p = (z[:, head(slot, S)] for z in now)
            p = jnp.exp(sc)
            ds = (p * d_p).astype(jnp.bfloat16)
            if pending:
                finish(*pending)
            pending = (QUARTERS * g + slot, p.astype(jnp.bfloat16), ds)
    finish(*pending)
    comm_point(1)
    cos_q, _, sin_q, cos_k, sin_k = (rope_ref[r] for r in range(5))
    for m, (src, cs, sn) in enumerate(((dq_s, cos_q, sin_q), (dk_s, cos_k, sin_k))):
        for h in range(H):
            lo, up = src[HP * h:HP * h + HALF, :], src[HP * h + HALF:HP * (h + 1), :]
            for n, z in enumerate((lo * cs + up * sn, up * cs - lo * sn)):
                wide, slim = QP * m + HP * h + HALF * n, D * m + HD * h + ROT * n
                dlin_s[wide:wide + HALF, :] = z
                dcmp_s[slim:slim + ROT, :] = z[:ROT]
    d_cmp = dcmp_s[...]
    dbias_ref[...] += fold(d_cmp)
    dcmp_b = d_cmp.astype(jnp.bfloat16)
    dlinb_s[...] = dlin_s[...].astype(jnp.bfloat16)
    e_t, keep, one_hot, _ = embed(tok_ref[0], len_ref[step], table_ref[...])
    xhat, rstd = norm_stats(e_t)
    g1, c1, _, _, _, _ = cols(vec_ref)
    h_t = spread(xhat * g1 + c1, sp, sx).astype(jnp.bfloat16)
    for sl in chunks(3 * D, 4 * LANES):
        dw_ref[:, sl] += dot(h_t, dcmp_b[sl, :], NT)
    d_h = pack(dot(w_ref[...], dlinb_s[...]), sy, sp)
    d_e = (norm_back(d_h, g1, xhat, rstd) + d_res) * keep
    dtab_ref[...] += dot(one_hot, d_e.astype(jnp.bfloat16), NT)
    dvec_ref[0] += fold(d_h * xhat)
    dvec_ref[1] += fold(d_h)

    @pl.when(step == pl.num_programs(0) - 1)
    def _():
        zero(sv_ref)
        sv_ref[:8, :] = sv_in[...]
        for r in range(5):
            sums = dvec_ref[r] if r < 2 else dbias_ref[head(r - 2, D), :]
            sv_ref[8 + r:9 + r, :] = lane_sums(sums)
        sv_ref[HALF:, :] = dtab_ref[...]
        for u, (_, out, sl) in zip(units, outs):
            settle(u, STAGES, f, c)
            out[:, sl] = u.fin[:out.shape[0], :]
            for stage in range(STAGES):
                for copy in stage_copies(u, stage, f, c):
                    copy.wait_send()


def enter(peers):
    barrier = pltpu.get_barrier_semaphore()
    for peer in peers:
        pl.semaphore_signal(barrier, inc=1, device_id=peer, device_id_type=MESH)
    pl.semaphore_wait(barrier, len(peers))


def copy_to(src, dst, sems, k, peer):
    return pltpu.make_async_remote_copy(src_ref=src, dst_ref=dst, send_sem=sems[0].at[k], recv_sem=sems[1].at[k], device_id=peer, device_id_type=MESH)


OWN_PUTS = (2, 4, 6, 1)
EARLY = 3
NEAR_CP = (2, 1, 3)
FAR = (2, 4, 6)


def grad_puts(src, dst, seqs, sems, loc, c):
    far = [copy_to(src.at[(c + d) % QUARTERS, seqs], dst.at[c, seqs], sems, d, {'cp': (c + d) % QUARTERS}) for d in NEAR_CP]
    return far, pltpu.make_async_copy(src.at[c, seqs], dst.at[c, seqs], loc)


def gather_kernel(w_ref, small_ref, tok_ref, g_ref, w_out, small_out, tok_out, g_out, w_send, w_recv, s_send, s_recv, t_send, t_recv, g_send, g_recv, loc_sem):
    f, c = lax.axis_index('fsdp'), lax.axis_index('cp')
    enter([{'fsdp': f ^ k} for k in range(1, PIECES)] + [{'cp': (c + d) % QUARTERS} for d in range(1, QUARTERS)])
    w_sems = (w_send, w_recv)
    smalls = [copy_to(small_ref, small_out.at[f], (s_send, s_recv), k, {'fsdp': f ^ k}) for k in range(1, PIECES)]
    smalls += [copy_to(tok_ref.at[(c + d) % QUARTERS], tok_out.at[c], (t_send, t_recv), d, {'cp': (c + d) % QUARTERS}) for d in range(1, QUARTERS)]
    puts = [copy_to(w_ref, w_out.at[f], w_sems, k, {'fsdp': f ^ k}) for k in OWN_PUTS]
    fwds = [copy_to(w_out.at[f ^ k], w_out.at[f ^ k], w_sems, k + 1, {'fsdp': f ^ 1}) for k in FAR]
    local = [pltpu.make_async_copy(a, b, loc_sem.at[m]) for m, (a, b) in enumerate(((w_ref, w_out.at[f]), (tok_ref.at[c], tok_out.at[c]), (small_ref, small_out.at[f])))]
    far, near = grad_puts(g_ref, g_out, pl.ds(0, EARLY), (g_send, g_recv), loc_sem.at[len(local)], c)
    local.append(near)
    for copy in puts + smalls + local + far:
        copy.start()
    for put, fwd in zip(puts, fwds):
        put.wait_recv()
        fwd.start()
    for copy in puts[len(FAR):] + smalls + fwds + far:
        copy.wait_recv()
    for copy in local:
        copy.wait()
    for copy in puts + smalls + fwds + far:
        copy.wait_send()


class Unit(typing.NamedTuple):
    src: typing.Any
    lanes: slice
    acc: typing.Any
    core: typing.Any
    xy: typing.Any
    xy2: typing.Any
    z: typing.Any
    fin: typing.Any
    send: typing.Any
    recv: typing.Any
    loc: typing.Any


STAGES = 5
POINTS = (0, 1, 3, 4, 6)
FFN_SPLITS = ((slice(0, 2 * LANES), slice(2 * LANES, D)), (slice(0, 8 * LANES), slice(8 * LANES, F)))


def reduce_peers(f, c):
    return [{'fsdp': f ^ k} for k in (1, 2, 4)] + [{'cp': (c + d) % QUARTERS} for d in range(1, QUARTERS)]


def loads(u, f):
    return [pltpu.make_async_copy(u.src.at[f ^ (2 * q), :, u.lanes], u.acc.at[q], u.loc.at[q]) for q in range(QUARTERS)]


def stage_copies(u, stage, f, c):
    rows = u.fin.shape[0]
    half, quarter = rows // 2, rows // QUARTERS
    lo, hi = pl.ds(0, half), pl.ds(half, half)
    own = lambda p: pl.ds(pl.multiple_of(p * quarter, 8), quarter)
    core, xp, yp = ({'fsdp': f ^ k} for k in (1, 2, 4))
    ac = u.acc
    if stage == 0:
        plan = [(u.src.at[(f ^ 1) ^ (2 * q), :, u.lanes], u.core.at[q], core) for q in (3, 1, 2, 0)]
    elif stage == 1:
        plan = [(ac.at[3, lo], u.xy.at[1], xp), (ac.at[3, hi], u.xy.at[3], yp), (ac.at[1, lo], u.xy.at[0], xp), (ac.at[2, hi], u.xy.at[2], yp)]
    elif stage == 2:
        plan = [(ac.at[2, lo], u.xy2.at[0], yp), (ac.at[1, hi], u.xy2.at[1], xp)]
    elif stage == 3:
        plan = [(ac.at[0, own((c + d) % QUARTERS)], u.z.at[d - 1], {'cp': (c + d) % QUARTERS}) for d in NEAR_CP]
    else:
        plan = [(u.fin.at[own(c)], u.fin.at[own(c)], {'cp': (c + d) % QUARTERS}) for d in NEAR_CP]
    return [copy_to(a, b, (u.send, u.recv), QUARTERS * stage + n, peer) for n, (a, b, peer) in enumerate(plan)]


def settle(u, stage, f, c):
    if not stage:
        return
    for copy in stage_copies(u, stage - 1, f, c):
        copy.wait_recv()
    rows = u.fin.shape[0]
    half, quarter = rows // 2, rows // QUARTERS
    lo, hi = slice(0, half), slice(half, rows)
    if stage == 1:
        for copy in loads(u, f):
            copy.wait()
        for q in (3, 1, 2, 0):
            u.acc[q] += u.core[q]
    elif stage == 2:
        for q, part, n in ((2, lo, 1), (1, hi, 3), (0, lo, 0), (0, hi, 2)):
            u.acc[q, part] += u.xy[n]
    elif stage == 3:
        u.acc[0, lo] += u.xy2[0]
        u.acc[0, hi] += u.xy2[1]
    elif stage == QUARTERS:
        mine = pl.ds(pl.multiple_of(c * quarter, 8), quarter)
        u.fin[mine] = (u.acc[0, mine] + u.z[0]) + (u.z[1] + u.z[2])


def reduce_kernel(dw_src, dwo_src, small, d_qkv, d_out, small_out, buf, r_small, *refs):
    n_unit = len(SPLITS) + 1
    refs = list(refs)
    b_send, b_recv, m_send, m_recv, loc_sem = refs[-5:]
    refs = refs[:-5]
    f, c = lax.axis_index('fsdp'), lax.axis_index('cp')
    enter(reduce_peers(f, c))
    outs = [(dwo_src, d_out, slice(0, D))] + [(dw_src, d_qkv, sl) for sl in SPLITS]
    units = [Unit(src, sl, *refs[m::n_unit], b_send.at[m], b_recv.at[m], loc_sem.at[m]) for m, (src, _, sl) in enumerate(outs)]
    steps = [{'fsdp': f ^ k} for k in (1, 2, 4)] + [{'cp': c ^ 1}, {'cp': c ^ 2}]
    small_puts = [copy_to(buf.at[t], r_small.at[t], (m_send, m_recv), t, peer) for t, peer in enumerate(steps)]
    for u in units:
        for copy in loads(u, f):
            copy.start()
    order = sorted((2 * stage + m, stage, m) for m in range(n_unit) for stage in range(1, STAGES + 1))
    for u in units:
        for copy in stage_copies(u, 0, f, c):
            copy.start()
    buf[0] = small[...]
    small_puts[0].start()
    small_at = {order[n_unit * t - 1]: t for t in range(1, STAGES + 1)}
    for op in order:
        _, stage, m = op
        settle(units[m], stage, f, c)
        if stage < STAGES:
            for copy in stage_copies(units[m], stage, f, c):
                copy.start()
        else:
            _, out, sl = outs[m]
            out[:, sl] = units[m].fin[:PV, :]
        if op in small_at:
            t = small_at[op]
            small_puts[t - 1].wait_recv()
            value = buf[t - 1] + r_small[t - 1]
            if t < STAGES:
                buf[t] = value
                small_puts[t].start()
            else:
                small_out[...] = value
    for copy in small_puts:
        copy.wait_send()
    for u in units:
        for stage in range(STAGES):
            for copy in stage_copies(u, stage, f, c):
                copy.wait_send()


def rope_tables():
    inv_freq = (1.0 / (ROPE_BASE ** (np.arange(0, HD, 2, dtype=np.float32) / np.float32(HD)))).astype(np.float32)
    angles = inv_freq[:, None] * np.arange(S, dtype=np.float32)[None, :]
    cos, sin = np.zeros((16, S), np.float32), np.zeros((16, S), np.float32)
    cos[:12], sin[:12] = np.cos(angles), np.sin(angles)
    scale = np.float32(HD ** -0.5)
    cos_q2 = cos * scale
    cos_q2[15] = 1.0
    cos_k2 = cos.copy()
    cos_k2[ROT:] = 1.0
    return np.stack([cos * scale, cos_q2, sin * scale, cos, sin, cos_k2])


def pad_heads(z):
    lead = z.shape[:-2]
    z = z.reshape(lead + (H, 2, HD // 2))
    z = jnp.pad(z, [(0, 0)] * len(lead) + [(0, 0), (0, 0), (0, 4)])
    return z.reshape(lead + (QP,))


def const(shape):
    return pl.BlockSpec(shape, lambda i, *_: (0,) * len(shape))


def per_seq(shape):
    return pl.BlockSpec((1,) + shape, lambda i, *_: (i,) + (0,) * len(shape))


def anys(n):
    return [pl.BlockSpec(memory_space=pl.ANY)] * n


def dma(*shape):
    return pltpu.SemaphoreType.DMA(shape)


def gather_all(w_loc, small, tok4, grad4):
    return pl.pallas_call(
        gather_kernel,
        in_specs=anys(4),
        out_specs=anys(4),
        out_shape=[b16(PIECES, *w_loc.shape), f32(PIECES, *small.shape), jax.ShapeDtypeStruct(tok4.shape, tok4.dtype), b16(*grad4.shape)],
        scratch_shapes=[dma(PIECES)] * 4 + [dma(QUARTERS)] * 5,
        compiler_params=pltpu.CompilerParams(collective_id=1, has_side_effects=True),
        name="gather_all",
    )(w_loc, small, tok4, grad4)


def unit_scratch(parts):
    v = lambda *shape: pltpu.VMEM(shape, jnp.float32)
    out = []
    for lead, div in ((4, 1), (4, 1), (4, 2), (2, 2), (3, 4)):
        out += [v(lead, r // div, n) for r, n in parts]
    return out + [v(r, n) for r, n in parts]


SPLITS = (slice(0, 6 * LANES), slice(6 * LANES, 3 * D))


def reduce_all(dw, dwo, small):
    vmem = pl.BlockSpec(memory_space=pltpu.VMEM)
    parts = [(PR, D)] + [(PR, sl.stop - sl.start) for sl in SPLITS]
    n = len(parts)
    scratch = [pltpu.VMEM((STAGES,) + small.shape, jnp.float32)] * 2 + unit_scratch(parts)
    scratch += [dma(n, QUARTERS * STAGES)] * 2 + [dma(STAGES)] * 2 + [dma(n, QUARTERS)]
    return pl.pallas_call(
        reduce_kernel,
        in_specs=anys(2) + [vmem],
        out_specs=[vmem] * 3,
        out_shape=[f32(PV, 3 * D), f32(PV, D), f32(*small.shape)],
        scratch_shapes=scratch,
        compiler_params=pltpu.CompilerParams(collective_id=2, has_side_effects=True, vmem_limit_bytes=58 * MIB),
        name="reduce_all",
    )(dw, dwo, small)


def call(kernel, cid, n, in_specs, out_specs, out_shape, scratch, flops, name, aliases={}):
    return pl.pallas_call(
        kernel,
        grid_spec=pltpu.PrefetchScalarGridSpec(num_scalar_prefetch=1, grid=(n,), in_specs=in_specs, out_specs=out_specs, scratch_shapes=scratch),
        out_shape=out_shape,
        compiler_params=pltpu.CompilerParams(dimension_semantics=("arbitrary",), vmem_limit_bytes=58 * MIB, collective_id=cid, has_side_effects=True),
        input_output_aliases=aliases,
        cost_estimate=pl.CostEstimate(flops=flops, bytes_accessed=20 * MIB, transcendentals=0),
        name=name,
    )


def f32(*shape):
    return jax.ShapeDtypeStruct(shape, jnp.float32)


def b16(*shape):
    return jax.ShapeDtypeStruct(shape, jnp.bfloat16)


def sv(*shape):
    return pltpu.VMEM(shape, jnp.float32)


def bv(*shape):
    return pltpu.VMEM(shape, jnp.bfloat16)


def solution(mesh):
    n_cp, n_fsdp = mesh.shape['cp'], mesh.shape['fsdp']

    def local_step(tokens, lengths, embed_table, layer_vecs, w_qkv, w_out, w_up, b_up, w_down, grad_out):
        n_seq, seq_loc = tokens.shape
        n = n_seq // n_cp
        cp_index, f_index = lax.axis_index('cp'), lax.axis_index('fsdp')
        rows_pad = lambda w: jnp.pad(w, ((0, PR - PV), (0, 0)))
        w_loc = jnp.concatenate([pad_heads(w_qkv[:, 0]), pad_heads(w_qkv[:, 1]), w_qkv[:, 2].reshape(PV, D)], axis=1)
        small = jnp.pad(jnp.concatenate([layer_vecs.reshape(-1), b_up]), (0, PIECES * LANES - 9 * PV - FV)).reshape(PIECES, LANES)
        grad4 = grad_out.reshape(n_cp, n, seq_loc, D)
        w_full, small, tok, grads = gather_all(rows_pad(w_loc), small, tokens.reshape(n_cp, n, seq_loc), grad4)
        w_full = w_full.reshape(DX, NQKV)
        small = small.reshape(n_fsdp, PIECES * LANES)
        vecs = small[:, :9 * PV].reshape(n_fsdp, 9, PV).transpose(1, 0, 2).reshape(9, D)
        bup = small[:, 9 * PV:9 * PV + FV].reshape(F, 1)
        tok = tok.transpose(1, 0, 2).reshape(n, 1, S)
        lens = lax.dynamic_slice(lengths, (cp_index * n,), (n,))
        table_t = jnp.pad(embed_table, ((0, VP - embed_table.shape[0]), (0, 0))).T
        vec_cols = jnp.concatenate([vecs[:2], vecs[5:], jnp.zeros((2, D), jnp.float32)], axis=0).T
        slot = np.arange(QP) % HP
        pad_one = jnp.asarray(np.stack([slot == HP - 1, slot >= HALF + ROT]).astype(np.float32))
        bias = jnp.concatenate([(pad_heads(vecs[2:4].reshape(2, H, HD)) + pad_one).reshape(2 * QP), vecs[4]])[:, None]
        rope = jnp.asarray(rope_tables())

        shared = [per_seq((1, S)), const((D, VP)), const((D, 8))]
        rope_spec = const(rope.shape)
        acts = [((QP, S), b16), ((QP, S), b16), ((S, QP), b16), ((S, QP), b16), ((D, S), f32), ((24, S), f32)]
        act_specs = [per_seq(shape) for shape, _ in acts]
        fwd = call(
            attn_fwd_kernel, 3, n,
            shared + [const((NQKV, 1)), rope_spec, const((DX, NQKV))] + anys(5),
            act_specs + anys(4),
            [kind(n, *shape) for shape, kind in acts] + [b16(PIECES, PR, D), b16(PIECES, PR, F), b16(PIECES, FV, D), b16(n_cp, n, seq_loc, D)],
            [bv(NQKV, DX), bv(QP, S), sv(D, S), sv(DX, S)] + [dma(3, PIECES)] * 2 + [dma(QUARTERS)] * 3,
            int(2e10), "attn_fwd", {11: 9})(lens, tok, table_t, vec_cols, bias, rope, w_full, rows_pad(w_out), rows_pad(w_up), w_down, grad4, grads)
        acts, (out_w, up_w, down_w, grads) = fwd[:6], fwd[6:]
        out_w, up_w, down_w = out_w.reshape(DX, D), up_w.reshape(DX, F), down_w.reshape(F, D)
        d_res, dwd, dwu, sv2, layer_out = call(
            ffn_kernel, 4, n,
            shared + [const((F, 1)), per_seq((D, S)), pl.BlockSpec((n_cp, 1, seq_loc, D), lambda i, *_: (0, i, 0, 0)), const((DX, D)), const((DX, F)), const((F, D))],
            [per_seq((D, S)), const((PIECES, FR, D)), const((DX, F)), const((8, D))] + anys(1),
            [f32(n, D, S), f32(PIECES, FR, D), f32(DX, F), f32(8, D), b16(n_seq, seq_loc, D)],
            [bv(D, DX), bv(F, DX), bv(D, F), bv(F, S), bv(F, S), sv(F, LANES), sv(4, D, LANES), sv(D, S), sv(DX, S), sv(DX, S), bv(2, S, D)]
            + [dma(n, QUARTERS)] * 2 + [dma(n)],
            int(4e10), "ffn")(lens, tok, table_t, vec_cols, bup, acts[4], grads, out_w, up_w, down_w)
        ffn_parts = [(r, sl.stop - sl.start) for r, splits in zip((FR, PR), FFN_SPLITS) for sl in splits]
        cut = lambda z: z.reshape(PIECES, PR, z.shape[1])
        dwo, dw, smalls, d_down_w, d_up_w = call(
            attn_bwd_kernel, 5, n,
            shared + [rope_spec] + act_specs + [per_seq((D, S)), const((DX, D)), const((DX, NQKV)), const((8, D))] + anys(2),
            [const((DX, D)), const((DX, 3 * D)), const((HALF + VP, D)), const((FV, D)), const((PV, F))],
            [f32(DX, D), f32(DX, 3 * D), f32(HALF + VP, D), f32(FV, D), f32(PV, F)],
            [bv(QP, S), sv(QP, S), sv(QP, S), sv(NQKV, S), sv(3 * D, S), bv(NQKV, S), sv(3 * D, LANES), sv(2, D, LANES), sv(VP, D), sv(D, S), sv(DX, S), sv(DX, S)]
            + unit_scratch(ffn_parts) + [dma(4, QUARTERS * STAGES)] * 2 + [dma(4, QUARTERS)],
            int(5e10), "attn_bwd")(lens, tok, table_t, vec_cols, rope, *acts, d_res, out_w, w_full, sv2, dwd, cut(dwu))
        d_qkv, d_out_w, smalls = reduce_all(cut(dw), cut(dwo), smalls)
        d_qkv = d_qkv.reshape((PV,) + w_qkv.shape[1:])
        all_vecs = jnp.concatenate([smalls[8:13], smalls[4:8]], axis=0)
        d_vecs = lax.dynamic_slice(all_vecs, (0, f_index * PV), (9, PV))
        d_bup = lax.dynamic_slice(smalls[:4].reshape(F), (f_index * FV,), (FV,))
        return layer_out, smalls[HALF:HALF + embed_table.shape[0]], d_vecs, d_qkv, d_out_w, d_up_w, d_bup, d_down_w

    rows = P('fsdp', None)
    in_specs = (P('fsdp', 'cp'), P('fsdp'), P(), P(None, 'fsdp'), P('fsdp', None, None, None), rows, rows, P('fsdp'), rows, P('fsdp', 'cp', None))
    out_specs = (P('fsdp', 'cp', None), P(), P(None, 'fsdp'), P('fsdp', None, None, None), rows, rows, P('fsdp'), rows)
    return jax.shard_map(local_step, mesh=mesh, in_specs=in_specs, out_specs=out_specs, check_vma=False)
```

```python
import functools
import typing

import numpy as np
import jax
import jax.numpy as jnp
from jax import lax
from jax.experimental import pallas as pl
from jax.experimental.pallas import tpu as pltpu
from jax.sharding import PartitionSpec as P

MASK_ID = 32
LN_EPS = 1e-5
ROPE_BASE = 10000.0
TRAIN_RATIO = 0.15 * 0.8
NEG_BIG = -1e30
D = 480
INV_D = 1.0 / D
H = 20
HD = 24
HP = 32
QP = H * HP
NQKV = 2 * QP + D
F = 1920
S = 256
VP = 40
PIECES = 8
PV = D // PIECES
PR = 64
DX = PIECES * PR
FR = 256
FV = F // PIECES
SQRT_HALF = 0.7071067811865476
INV_SQRT_2PI = 0.3989422804014327
LANES = 128
HALF = 16
ROT = HD // 2
MIB = 2 ** 20
MESH = pl.DeviceIdType.MESH
QUARTERS = 4
GROUPS = H // QUARTERS

NN = (((1,), (0,)), ((), ()))
NT = (((1,), (1,)), ((), ()))


def dot(a, b, dims=NN):
    return lax.dot_general(a, b, dims, preferred_element_type=jnp.float32)


def eye(n):
    return (lax.broadcasted_iota(jnp.int32, (n, n), 0) == lax.broadcasted_iota(jnp.int32, (n, n), 1)).astype(jnp.float32).astype(jnp.bfloat16)


def fold(z):
    return z[:, :LANES] + z[:, LANES:]


def col_sum(z):
    return jnp.sum(z, axis=0, keepdims=True)


def chunks(total, width):
    return [slice(j, min(j + width, total)) for j in range(0, total, width)]


def zero(*refs):
    for ref in refs:
        ref[...] = jnp.zeros_like(ref)


def head(h, width=None):
    width = HP if width is None else width
    return slice(width * h, width * (h + 1))


def side_by_side(g, block):
    return jnp.concatenate([place(block(QUARTERS * g + slot), slot) for slot in range(QUARTERS)], axis=1)


def cols(ref):
    return [ref[:, j:j + 1] for j in range(6)]


def embed(tok, length, table_t):
    pos = lax.broadcasted_iota(jnp.int32, (1, S), 1)
    is_mask = tok == MASK_ID
    valid = pos < length
    n_mask = jnp.sum(is_mask.astype(jnp.float32), axis=1, keepdims=True)
    len_f = jnp.full((1, 1), length, jnp.int32).astype(jnp.float32)
    scale = (1.0 - TRAIN_RATIO) / (1.0 - n_mask / len_f)
    keep = jnp.where(is_mask | jnp.logical_not(valid), 0.0, scale)
    one_hot = (lax.broadcasted_iota(jnp.int32, (VP, S), 0) == tok).astype(jnp.float32).astype(jnp.bfloat16)
    return dot(table_t, one_hot) * keep, keep, one_hot, valid


def norm_stats(z):
    mean = col_sum(z) * INV_D
    cen = z - mean
    var = col_sum(cen * cen) * INV_D
    rstd = lax.rsqrt(var + LN_EPS)
    return cen * rstd, rstd


def norm_back(d_out, gain, xhat, rstd):
    d_hat = d_out * gain
    m1 = col_sum(d_hat) * INV_D
    m2 = col_sum(d_hat * xhat) * INV_D
    return rstd * (d_hat - m1 - xhat * m2)


def spread(z, src, dst):
    src[...] = z
    for j in range(PIECES):
        dst[PR * j:PR * j + PV, :] = src[PV * j:PV * (j + 1), :]
    return dst[...]


def pack(z, src, dst):
    src[...] = z
    for j in range(PIECES):
        dst[PV * j:PV * (j + 1), :] = src[PR * j:PR * j + PV, :]
    return dst[...]


def split3(z):
    parts = []
    for _ in range(3):
        parts.append(z.astype(jnp.bfloat16))
        z = z - parts[-1].astype(jnp.float32)
    return parts


def lane_sums(acc):
    ones = jnp.ones((8, LANES), jnp.bfloat16)
    hi, mid, lo = (dot(ones, part, NT)[:1] for part in split3(acc))
    return hi + (mid + lo)


def minus_rows(block, first, value):
    row = lax.broadcasted_iota(jnp.int32, block.shape, 0)
    for n, part in enumerate(split3(-value)):
        block = jnp.where(row == first + n, part.astype(jnp.float32), block)
    return block.astype(jnp.bfloat16)


def flip(w_ref, out, width):
    ident = eye(LANES)
    for sl in chunks(width, LANES):
        n = sl.stop - sl.start
        out[sl, :] = dot(ident[:n, :n], w_ref[:, sl], NT).astype(jnp.bfloat16)


def place(rows, slot):
    parts = []
    if slot:
        parts.append(jnp.zeros((HP * slot, S), rows.dtype))
    parts.append(rows)
    if slot < 3:
        parts.append(jnp.zeros((HP * (3 - slot), S), rows.dtype))
    return jnp.concatenate(parts, axis=0)


def rope_store(lin, out, base, ca, cb, sn):
    for h in range(H):
        lo, up = lin[HP * h:HP * h + HALF], lin[HP * h + HALF:HP * (h + 1)]
        out[0, base + HP * h:base + HP * h + HALF, :] = (lo * ca - up * sn).astype(jnp.bfloat16)
        out[0, base + HP * h + HALF:base + HP * (h + 1), :] = (up * cb + lo * sn).astype(jnp.bfloat16)


def attn_fwd_kernel(len_ref, tok_ref, table_ref, vec_ref, bias_ref, rope_ref, w_ref, wo_loc, wu_loc, wd_loc, g_loc, g_part,
                    q_out, k_out, krow_out, vrow_out, o_out, lse_out, wo_all, wu_all, wd_all, g_all,
                    wt, v_t, sp, sx, w_send, w_recv, g_send, g_recv, loc_sem):
    step = pl.program_id(0)
    last = pl.num_programs(0) - 1
    f, c = lax.axis_index('fsdp'), lax.axis_index('cp')
    pairs = [(wo_loc, wo_all), (wu_loc, wu_all), (wd_loc, wd_all)]
    g_puts, g_near = grad_puts(g_loc, g_all, pl.ds(EARLY, g_loc.shape[1] - EARLY), (g_send, g_recv), loc_sem.at[len(pairs)], c)
    w_puts = [copy_to(loc, full.at[f], (w_send.at[m], w_recv.at[m]), k, {'fsdp': f ^ k}) for m, (loc, full) in enumerate(pairs) for k in OWN_PUTS]
    w_fwds = [copy_to(full.at[f ^ k], full.at[f ^ k], (w_send.at[m], w_recv.at[m]), k + 1, {'fsdp': f ^ 1}) for m, (_, full) in enumerate(pairs) for k in FAR]
    local = [pltpu.make_async_copy(loc, full.at[f], loc_sem.at[m]) for m, (loc, full) in enumerate(pairs)]
    local.append(g_near)

    @pl.when(step == 0)
    def _():
        enter([{'fsdp': f ^ k} for k in OWN_PUTS] + [{'cp': (c + d) % QUARTERS} for d in range(1, QUARTERS)])
        for copy in w_puts + g_puts + local:
            copy.start()
        zero(sx)
        flip(w_ref, wt, NQKV)

    @pl.when(step == last - 1)
    def _():
        for m in range(len(pairs)):
            for n, k in enumerate(OWN_PUTS):
                if k in FAR:
                    w_puts[m * len(OWN_PUTS) + n].wait_recv()
        for copy in w_fwds:
            copy.start()

    e_t, _, _, valid = embed(tok_ref[0], len_ref[step], table_ref[...])
    xhat, _ = norm_stats(e_t)
    g1, c1, _, _, _, _ = cols(vec_ref)
    h_t = spread(xhat * g1 + c1, sp, sx).astype(jnp.bfloat16)
    mask_row = jnp.where(valid, 0.0, NEG_BIG)
    cos_q, cos_q2, sin_q, cos_k, sin_k, cos_k2 = (rope_ref[r] for r in range(6))
    cos_k2 = jnp.where(lax.broadcasted_iota(jnp.int32, (HALF, S), 0) == HALF - 1, mask_row, cos_k2)
    rope_store(dot(wt[:QP, :], h_t) + bias_ref[:QP, :], q_out, 0, cos_q, cos_q2, sin_q)
    rope_store(dot(wt[QP:2 * QP, :], h_t) + bias_ref[QP:2 * QP, :], k_out, 0, cos_k, cos_k2, sin_k)
    v_lin = dot(wt[2 * QP:, :], h_t) + bias_ref[2 * QP:, :]
    pad = (lax.broadcasted_iota(jnp.int32, (HP - HD, S), 0) < 3).astype(jnp.float32)
    for h in range(H):
        v_t[head(h), :] = jnp.concatenate([v_lin[head(h, HD)], pad], axis=0).astype(jnp.bfloat16)
    ident = eye(S)
    krow_out[0] = dot(ident, k_out[0], NT).astype(jnp.bfloat16)
    vrow_out[0] = dot(ident, v_t[...], NT).astype(jnp.bfloat16)
    def scores(g):
        return dot(krow_out[0, :, head(g, LANES)], side_by_side(g, lambda h: q_out[0, head(h), :]))

    def finish(h, top, tot, p):
        o_h = dot(v_t[head(h), :], p)
        o_out[0, head(h, HD), :] = o_h[:HD] / tot
        lse_out[0, h:h + 1, :] = top + jnp.log(tot)

    pending = None
    ahead = scores(0)
    for g in range(GROUPS):
        now = ahead
        if g + 1 < GROUPS:
            ahead = scores(g + 1)
        for slot in range(QUARTERS):
            sc = now[:, head(slot, S)]
            top = jnp.max(sc, axis=0, keepdims=True)
            p = jnp.exp(sc - top)
            if pending:
                finish(*pending)
            pending = (QUARTERS * g + slot, top, col_sum(p), p.astype(jnp.bfloat16))
    finish(*pending)

    @pl.when(step == last)
    def _():
        for n, copy in enumerate(w_puts):
            if OWN_PUTS[n % len(OWN_PUTS)] not in FAR:
                copy.wait_recv()
        for copy in w_fwds + g_puts:
            copy.wait_recv()
        for copy in local:
            copy.wait()
        for copy in w_puts + w_fwds + g_puts:
            copy.wait_send()


def ffn_kernel(len_ref, tok_ref, table_ref, vec_ref, bup_ref, o_ref, g_ref, wo_ref, wu_ref, wd_ref,
               dres_ref, dwd_ref, dwu_ref, sv_ref, out_all, wot, wut, wdt, gelu_s, dup_s, dbup_ref, dvec_ref, sp, sx, sy, obuf, o_send, o_recv, loc_sem):
    step = pl.program_id(0)
    n_step = pl.num_programs(0)
    c = lax.axis_index('cp')
    rows = S // QUARTERS

    def out_puts(i):
        slot = lax.rem(i, 2)
        part = lambda p: obuf.at[slot, pl.ds(pl.multiple_of(p * rows, rows), rows)]
        dst = out_all.at[c * n_step + i]
        far = [copy_to(part((c + d) % QUARTERS), dst, (o_send.at[i], o_recv.at[i]), d, {'cp': (c + d) % QUARTERS}) for d in NEAR_CP]
        return far, pltpu.make_async_copy(part(c), dst, loc_sem.at[i])

    @pl.when(step == 0)
    def _():
        enter([{'cp': (c + d) % QUARTERS} for d in range(1, QUARTERS)])
        zero(sx, dwd_ref, dwu_ref, dbup_ref, dvec_ref)
        flip(wo_ref, wot, D)
        flip(wd_ref, wdt, D)
        flip(wu_ref, wut, F)

    @pl.when(step >= 2)
    def _():
        far, near = out_puts(step - 2)
        near.wait()
        for copy in far:
            copy.wait_send()

    _, _, b_o, gain2, bias2, b_down = cols(vec_ref)
    e_t, _, _, _ = embed(tok_ref[0], len_ref[step], table_ref[...])
    o_x = spread(o_ref[0], sp, sx).astype(jnp.bfloat16)
    x1 = e_t + dot(wot[...], o_x) + b_o
    xhat, rstd = norm_stats(x1)
    n_t = spread(xhat * gain2 + bias2, sp, sx).astype(jnp.bfloat16)
    g_t32 = dot(eye(D), g_ref[...].reshape(S, D), NT)
    g_t = g_t32.astype(jnp.bfloat16)
    def products(sl):
        return dot(wut[sl, :], n_t), dot(wd_ref[sl, :], g_t)

    parts = chunks(F, D)
    ahead = products(parts[0])
    for n, sl in enumerate(parts):
        up, d_gelu = ahead
        if n + 1 < len(parts):
            ahead = products(parts[n + 1])
        up = up + bup_ref[sl, :]
        cdf = 0.5 * (1.0 + lax.erf(up * SQRT_HALF))
        pdf = jnp.exp(up * up * -0.5) * INV_SQRT_2PI
        gelu_s[sl, :] = (up * cdf).astype(jnp.bfloat16)
        d_up = d_gelu * (cdf + up * pdf)
        dup_s[sl, :] = d_up.astype(jnp.bfloat16)
        dbup_ref[sl, :] += fold(d_up)
    out_t = (x1 + dot(wdt[...], gelu_s[...]) + b_down).astype(jnp.bfloat16)
    obuf[lax.rem(step, 2)] = dot(eye(S), out_t, NT).astype(jnp.bfloat16)
    d_down = dot(gelu_s[...], g_t, NT)
    for j in range(PIECES):
        dwd_ref[j, :FV, :] += d_down[head(j, FV)]
    far, near = out_puts(step)
    for copy in far + [near]:
        copy.start()
    for sl in chunks(F, 4 * LANES):
        dwu_ref[:, sl] += dot(n_t, dup_s[sl, :], NT)
    d_n = pack(dot(wu_ref[...], dup_s[...]), sy, sp)
    d_res = g_t32 + norm_back(d_n, gain2, xhat, rstd)
    dres_ref[0] = d_res
    for r, z in enumerate((d_res, d_n * xhat, d_n, g_t32)):
        dvec_ref[r] += fold(z)

    @pl.when(step == n_step - 1)
    def _():
        for r in range(4):
            sv_ref[r:r + 1, :] = lane_sums(dbup_ref[head(r, D), :])
            sv_ref[r + 4:r + 5, :] = lane_sums(dvec_ref[r])
        for back in range(2):
            far, near = out_puts(step - back)
            near.wait()
            for copy in far:
                copy.wait_send()

        def drain(i, carry):
            for copy in out_puts(i)[0]:
                copy.wait_recv()
            return carry

        lax.fori_loop(0, n_step, drain, 0)


def attn_bwd_kernel(len_ref, tok_ref, table_ref, vec_ref, rope_ref, q_ref, k_ref, krow_ref, vrow_ref, o_ref, lse_ref, dres_ref, wo_ref, w_ref, sv_in, dwd_src, dwu_src,
                    dwo_ref, dw_ref, sv_ref, pd_ref, pu_ref, da_s, dq_s, dk_s, dlin_s, dcmp_s, dlinb_s, dbias_ref, dvec_ref, dtab_ref, sp, sx, sy, *comm):
    step = pl.program_id(0)
    f, c = lax.axis_index('fsdp'), lax.axis_index('cp')
    refs = list(comm)
    b_send, b_recv, loc_sem = refs[-3:]
    outs = [(dwd_src, pd_ref, sl) for sl in FFN_SPLITS[0]] + [(dwu_src, pu_ref, sl) for sl in FFN_SPLITS[1]]
    units = [Unit(src, sl, *refs[m:-3:len(outs)], b_send.at[m], b_recv.at[m], loc_sem.at[m]) for m, (src, _, sl) in enumerate(outs)]

    def advance(*todo):
        for m, stage in todo:
            settle(units[m], stage, f, c)
        for m, stage in todo:
            for copy in stage_copies(units[m], stage, f, c):
                copy.start()

    def comm_point(late):
        for i in range(H // 2):
            point = 2 * i + late
            todo = [(m, stage) for m in range(len(units)) for stage, at in enumerate(POINTS) if stage and at + 3 * m == point]
            if todo:
                pl.when(step == i)(functools.partial(advance, *todo))

    @pl.when(step == 0)
    def _():
        enter(reduce_peers(f, c))
        for u in units:
            for copy in loads(u, f):
                copy.start()
        advance(*((m, 0) for m in range(len(units))))
        zero(sx, dwo_ref, dw_ref, dtab_ref, dbias_ref, dvec_ref)

    comm_point(0)

    d_res = dres_ref[0]
    d_res_b = d_res.astype(jnp.bfloat16)
    dwo_ref[...] += dot(spread(o_ref[0], sp, sx).astype(jnp.bfloat16), d_res_b, NT)
    d_attn = pack(dot(wo_ref[...], d_res_b), sy, sp)
    prod = d_attn * o_ref[0]
    pad = jnp.zeros((HP - HD, S), jnp.float32)
    for h in range(H):
        delta = col_sum(prod[head(h, HD)])
        da_s[head(h), :] = jnp.concatenate([d_attn[head(h, HD)], minus_rows(pad, 0, delta).astype(jnp.float32)], axis=0).astype(jnp.bfloat16)
    def q_block(h):
        q_h = q_ref[0, head(h), :]
        q_up = minus_rows(q_h[HALF:].astype(jnp.float32), ROT, lse_ref[0, h:h + 1, :])
        return jnp.concatenate([q_h[:HALF], q_up], axis=0)

    def scores(g):
        lanes = head(g, LANES)
        return dot(krow_ref[0, :, lanes], side_by_side(g, q_block)), dot(vrow_ref[0, :, lanes], side_by_side(g, lambda h: da_s[head(h), :]))

    def finish(h, p, ds):
        rows = head(h)
        dq_s[rows, :] = dot(k_ref[0, rows, :], ds)
        dk_s[rows, :] = dot(q_ref[0, rows, :], ds, NT)
        d_v = dot(da_s[rows, :], p, NT)[:HD]
        dlin_s[2 * QP + HD * h:2 * QP + HD * (h + 1), :] = d_v
        dcmp_s[2 * D + HD * h:2 * D + HD * (h + 1), :] = d_v

    pending = None
    ahead = scores(0)
    for g in range(GROUPS):
        now = ahead
        if g + 1 < GROUPS:
            ahead = scores(g + 1)
        for slot in range(QUARTERS):
            sc, d_p = (z[:, head(slot, S)] for z in now)
            p = jnp.exp(sc)
            ds = (p * d_p).astype(jnp.bfloat16)
            if pending:
                finish(*pending)
            pending = (QUARTERS * g + slot, p.astype(jnp.bfloat16), ds)
    finish(*pending)
    comm_point(1)
    cos_q, _, sin_q, cos_k, sin_k = (rope_ref[r] for r in range(5))
    for m, (src, cs, sn) in enumerate(((dq_s, cos_q, sin_q), (dk_s, cos_k, sin_k))):
        for h in range(H):
            lo, up = src[HP * h:HP * h + HALF, :], src[HP * h + HALF:HP * (h + 1), :]
            for n, z in enumerate((lo * cs + up * sn, up * cs - lo * sn)):
                wide, slim = QP * m + HP * h + HALF * n, D * m + HD * h + ROT * n
                dlin_s[wide:wide + HALF, :] = z
                dcmp_s[slim:slim + ROT, :] = z[:ROT]
    d_cmp = dcmp_s[...]
    dbias_ref[...] += fold(d_cmp)
    dcmp_b = d_cmp.astype(jnp.bfloat16)
    dlinb_s[...] = dlin_s[...].astype(jnp.bfloat16)
    e_t, keep, one_hot, _ = embed(tok_ref[0], len_ref[step], table_ref[...])
    xhat, rstd = norm_stats(e_t)
    g1, c1, _, _, _, _ = cols(vec_ref)
    h_t = spread(xhat * g1 + c1, sp, sx).astype(jnp.bfloat16)
    for sl in chunks(3 * D, 4 * LANES):
        dw_ref[:, sl] += dot(h_t, dcmp_b[sl, :], NT)
    d_h = pack(dot(w_ref[...], dlinb_s[...]), sy, sp)
    d_e = (norm_back(d_h, g1, xhat, rstd) + d_res) * keep
    dtab_ref[...] += dot(one_hot, d_e.astype(jnp.bfloat16), NT)
    dvec_ref[0] += fold(d_h * xhat)
    dvec_ref[1] += fold(d_h)

    @pl.when(step == pl.num_programs(0) - 1)
    def _():
        zero(sv_ref)
        sv_ref[:8, :] = sv_in[...]
        for r in range(5):
            sums = dvec_ref[r] if r < 2 else dbias_ref[head(r - 2, D), :]
            sv_ref[8 + r:9 + r, :] = lane_sums(sums)
        sv_ref[HALF:, :] = dtab_ref[...]
        for u, (_, out, sl) in zip(units, outs):
            settle(u, STAGES, f, c)
            out[:, sl] = u.fin[:out.shape[0], :]
            for stage in range(STAGES):
                for copy in stage_copies(u, stage, f, c):
                    copy.wait_send()


def enter(peers):
    barrier = pltpu.get_barrier_semaphore()
    for peer in peers:
        pl.semaphore_signal(barrier, inc=1, device_id=peer, device_id_type=MESH)
    pl.semaphore_wait(barrier, len(peers))


def copy_to(src, dst, sems, k, peer):
    return pltpu.make_async_remote_copy(src_ref=src, dst_ref=dst, send_sem=sems[0].at[k], recv_sem=sems[1].at[k], device_id=peer, device_id_type=MESH)


OWN_PUTS = (2, 4, 6, 1)
EARLY = 2
NEAR_CP = (2, 1, 3)
FAR = (2, 4, 6)


def grad_puts(src, dst, seqs, sems, loc, c):
    far = [copy_to(src.at[(c + d) % QUARTERS, seqs], dst.at[c, seqs], sems, d, {'cp': (c + d) % QUARTERS}) for d in NEAR_CP]
    return far, pltpu.make_async_copy(src.at[c, seqs], dst.at[c, seqs], loc)


def gather_kernel(w_ref, small_ref, tok_ref, g_ref, w_out, small_out, tok_out, g_out, w_send, w_recv, s_send, s_recv, t_send, t_recv, g_send, g_recv, loc_sem):
    f, c = lax.axis_index('fsdp'), lax.axis_index('cp')
    enter([{'fsdp': f ^ k} for k in range(1, PIECES)] + [{'cp': (c + d) % QUARTERS} for d in range(1, QUARTERS)])
    w_sems = (w_send, w_recv)
    smalls = [copy_to(small_ref, small_out.at[f], (s_send, s_recv), k, {'fsdp': f ^ k}) for k in range(1, PIECES)]
    smalls += [copy_to(tok_ref.at[(c + d) % QUARTERS], tok_out.at[c], (t_send, t_recv), d, {'cp': (c + d) % QUARTERS}) for d in range(1, QUARTERS)]
    puts = [copy_to(w_ref, w_out.at[f], w_sems, k, {'fsdp': f ^ k}) for k in OWN_PUTS]
    fwds = [copy_to(w_out.at[f ^ k], w_out.at[f ^ k], w_sems, k + 1, {'fsdp': f ^ 1}) for k in FAR]
    local = [pltpu.make_async_copy(a, b, loc_sem.at[m]) for m, (a, b) in enumerate(((w_ref, w_out.at[f]), (tok_ref.at[c], tok_out.at[c]), (small_ref, small_out.at[f])))]
    far, near = grad_puts(g_ref, g_out, pl.ds(0, EARLY), (g_send, g_recv), loc_sem.at[len(local)], c)
    local.append(near)
    for copy in puts + smalls + local + far:
        copy.start()
    for put, fwd in zip(puts, fwds):
        put.wait_recv()
        fwd.start()
    for copy in puts[len(FAR):] + smalls + fwds + far:
        copy.wait_recv()
    for copy in local:
        copy.wait()
    for copy in puts + smalls + fwds + far:
        copy.wait_send()


class Unit(typing.NamedTuple):
    src: typing.Any
    lanes: slice
    acc: typing.Any
    core: typing.Any
    xy: typing.Any
    xy2: typing.Any
    z: typing.Any
    fin: typing.Any
    send: typing.Any
    recv: typing.Any
    loc: typing.Any


STAGES = 5
POINTS = (0, 1, 3, 4, 6)
FFN_SPLITS = ((slice(0, 2 * LANES), slice(2 * LANES, D)), (slice(0, 8 * LANES), slice(8 * LANES, F)))


def reduce_peers(f, c):
    return [{'fsdp': f ^ k} for k in (1, 2, 4)] + [{'cp': (c + d) % QUARTERS} for d in range(1, QUARTERS)]


def loads(u, f):
    return [pltpu.make_async_copy(u.src.at[f ^ (2 * q), :, u.lanes], u.acc.at[q], u.loc.at[q]) for q in range(QUARTERS)]


def stage_copies(u, stage, f, c):
    rows = u.fin.shape[0]
    half, quarter = rows // 2, rows // QUARTERS
    lo, hi = pl.ds(0, half), pl.ds(half, half)
    own = lambda p: pl.ds(pl.multiple_of(p * quarter, 8), quarter)
    core, xp, yp = ({'fsdp': f ^ k} for k in (1, 2, 4))
    ac = u.acc
    if stage == 0:
        plan = [(u.src.at[(f ^ 1) ^ (2 * q), :, u.lanes], u.core.at[q], core) for q in (3, 1, 2, 0)]
    elif stage == 1:
        plan = [(ac.at[3, lo], u.xy.at[1], xp), (ac.at[3, hi], u.xy.at[3], yp), (ac.at[1, lo], u.xy.at[0], xp), (ac.at[2, hi], u.xy.at[2], yp)]
    elif stage == 2:
        plan = [(ac.at[2, lo], u.xy2.at[0], yp), (ac.at[1, hi], u.xy2.at[1], xp)]
    elif stage == 3:
        plan = [(ac.at[0, own((c + d) % QUARTERS)], u.z.at[d - 1], {'cp': (c + d) % QUARTERS}) for d in NEAR_CP]
    else:
        plan = [(u.fin.at[own(c)], u.fin.at[own(c)], {'cp': (c + d) % QUARTERS}) for d in NEAR_CP]
    return [copy_to(a, b, (u.send, u.recv), QUARTERS * stage + n, peer) for n, (a, b, peer) in enumerate(plan)]


def settle(u, stage, f, c):
    if not stage:
        return
    for copy in stage_copies(u, stage - 1, f, c):
        copy.wait_recv()
    rows = u.fin.shape[0]
    half, quarter = rows // 2, rows // QUARTERS
    lo, hi = slice(0, half), slice(half, rows)
    if stage == 1:
        for copy in loads(u, f):
            copy.wait()
        for q in (3, 1, 2, 0):
            u.acc[q] += u.core[q]
    elif stage == 2:
        for q, part, n in ((2, lo, 1), (1, hi, 3), (0, lo, 0), (0, hi, 2)):
            u.acc[q, part] += u.xy[n]
    elif stage == 3:
        u.acc[0, lo] += u.xy2[0]
        u.acc[0, hi] += u.xy2[1]
    elif stage == QUARTERS:
        mine = pl.ds(pl.multiple_of(c * quarter, 8), quarter)
        u.fin[mine] = (u.acc[0, mine] + u.z[0]) + (u.z[1] + u.z[2])


def reduce_kernel(dw_src, dwo_src, small, d_qkv, d_out, small_out, buf, r_small, *refs):
    n_unit = len(SPLITS) + 1
    refs = list(refs)
    b_send, b_recv, m_send, m_recv, loc_sem = refs[-5:]
    refs = refs[:-5]
    f, c = lax.axis_index('fsdp'), lax.axis_index('cp')
    enter(reduce_peers(f, c))
    outs = [(dwo_src, d_out, slice(0, D))] + [(dw_src, d_qkv, sl) for sl in SPLITS]
    units = [Unit(src, sl, *refs[m::n_unit], b_send.at[m], b_recv.at[m], loc_sem.at[m]) for m, (src, _, sl) in enumerate(outs)]
    steps = [{'fsdp': f ^ k} for k in (1, 2, 4)] + [{'cp': c ^ 1}, {'cp': c ^ 2}]
    small_puts = [copy_to(buf.at[t], r_small.at[t], (m_send, m_recv), t, peer) for t, peer in enumerate(steps)]
    for u in units:
        for copy in loads(u, f):
            copy.start()
    order = sorted((2 * stage + m, stage, m) for m in range(n_unit) for stage in range(1, STAGES + 1))
    for u in units:
        for copy in stage_copies(u, 0, f, c):
            copy.start()
    buf[0] = small[...]
    small_puts[0].start()
    small_at = {order[n_unit * t - 1]: t for t in range(1, STAGES + 1)}
    for op in order:
        _, stage, m = op
        settle(units[m], stage, f, c)
        if stage < STAGES:
            for copy in stage_copies(units[m], stage, f, c):
                copy.start()
        else:
            _, out, sl = outs[m]
            out[:, sl] = units[m].fin[:PV, :]
        if op in small_at:
            t = small_at[op]
            small_puts[t - 1].wait_recv()
            value = buf[t - 1] + r_small[t - 1]
            if t < STAGES:
                buf[t] = value
                small_puts[t].start()
            else:
                small_out[...] = value
    for copy in small_puts:
        copy.wait_send()
    for u in units:
        for stage in range(STAGES):
            for copy in stage_copies(u, stage, f, c):
                copy.wait_send()


def rope_tables():
    inv_freq = (1.0 / (ROPE_BASE ** (np.arange(0, HD, 2, dtype=np.float32) / np.float32(HD)))).astype(np.float32)
    angles = inv_freq[:, None] * np.arange(S, dtype=np.float32)[None, :]
    cos, sin = np.zeros((16, S), np.float32), np.zeros((16, S), np.float32)
    cos[:12], sin[:12] = np.cos(angles), np.sin(angles)
    scale = np.float32(HD ** -0.5)
    cos_q2 = cos * scale
    cos_q2[15] = 1.0
    cos_k2 = cos.copy()
    cos_k2[ROT:] = 1.0
    return np.stack([cos * scale, cos_q2, sin * scale, cos, sin, cos_k2])


def pad_heads(z):
    lead = z.shape[:-2]
    z = z.reshape(lead + (H, 2, HD // 2))
    z = jnp.pad(z, [(0, 0)] * len(lead) + [(0, 0), (0, 0), (0, 4)])
    return z.reshape(lead + (QP,))


def const(shape):
    return pl.BlockSpec(shape, lambda i, *_: (0,) * len(shape))


def per_seq(shape):
    return pl.BlockSpec((1,) + shape, lambda i, *_: (i,) + (0,) * len(shape))


def anys(n):
    return [pl.BlockSpec(memory_space=pl.ANY)] * n


def dma(*shape):
    return pltpu.SemaphoreType.DMA(shape)


def gather_all(w_loc, small, tok4, grad4):
    return pl.pallas_call(
        gather_kernel,
        in_specs=anys(4),
        out_specs=anys(4),
        out_shape=[b16(PIECES, *w_loc.shape), f32(PIECES, *small.shape), jax.ShapeDtypeStruct(tok4.shape, tok4.dtype), b16(*grad4.shape)],
        scratch_shapes=[dma(PIECES)] * 4 + [dma(QUARTERS)] * 5,
        compiler_params=pltpu.CompilerParams(collective_id=1, has_side_effects=True),
        name="gather_all",
    )(w_loc, small, tok4, grad4)


def unit_scratch(parts):
    v = lambda *shape: pltpu.VMEM(shape, jnp.float32)
    out = []
    for lead, div in ((4, 1), (4, 1), (4, 2), (2, 2), (3, 4)):
        out += [v(lead, r // div, n) for r, n in parts]
    return out + [v(r, n) for r, n in parts]


SPLITS = (slice(0, 6 * LANES), slice(6 * LANES, 3 * D))


def reduce_all(dw, dwo, small):
    vmem = pl.BlockSpec(memory_space=pltpu.VMEM)
    parts = [(PR, D)] + [(PR, sl.stop - sl.start) for sl in SPLITS]
    n = len(parts)
    scratch = [pltpu.VMEM((STAGES,) + small.shape, jnp.float32)] * 2 + unit_scratch(parts)
    scratch += [dma(n, QUARTERS * STAGES)] * 2 + [dma(STAGES)] * 2 + [dma(n, QUARTERS)]
    return pl.pallas_call(
        reduce_kernel,
        in_specs=anys(2) + [vmem],
        out_specs=[vmem] * 3,
        out_shape=[f32(PV, 3 * D), f32(PV, D), f32(*small.shape)],
        scratch_shapes=scratch,
        compiler_params=pltpu.CompilerParams(collective_id=2, has_side_effects=True, vmem_limit_bytes=58 * MIB),
        name="reduce_all",
    )(dw, dwo, small)


def call(kernel, cid, n, in_specs, out_specs, out_shape, scratch, flops, name, aliases={}):
    return pl.pallas_call(
        kernel,
        grid_spec=pltpu.PrefetchScalarGridSpec(num_scalar_prefetch=1, grid=(n,), in_specs=in_specs, out_specs=out_specs, scratch_shapes=scratch),
        out_shape=out_shape,
        compiler_params=pltpu.CompilerParams(dimension_semantics=("arbitrary",), vmem_limit_bytes=58 * MIB, collective_id=cid, has_side_effects=True),
        input_output_aliases=aliases,
        cost_estimate=pl.CostEstimate(flops=flops, bytes_accessed=20 * MIB, transcendentals=0),
        name=name,
    )


def f32(*shape):
    return jax.ShapeDtypeStruct(shape, jnp.float32)


def b16(*shape):
    return jax.ShapeDtypeStruct(shape, jnp.bfloat16)


def sv(*shape):
    return pltpu.VMEM(shape, jnp.float32)


def bv(*shape):
    return pltpu.VMEM(shape, jnp.bfloat16)


def solution(mesh):
    n_cp, n_fsdp = mesh.shape['cp'], mesh.shape['fsdp']

    def local_step(tokens, lengths, embed_table, layer_vecs, w_qkv, w_out, w_up, b_up, w_down, grad_out):
        n_seq, seq_loc = tokens.shape
        n = n_seq // n_cp
        cp_index, f_index = lax.axis_index('cp'), lax.axis_index('fsdp')
        rows_pad = lambda w: jnp.pad(w, ((0, PR - PV), (0, 0)))
        w_loc = jnp.concatenate([pad_heads(w_qkv[:, 0]), pad_heads(w_qkv[:, 1]), w_qkv[:, 2].reshape(PV, D)], axis=1)
        small = jnp.pad(jnp.concatenate([layer_vecs.reshape(-1), b_up]), (0, PIECES * LANES - 9 * PV - FV)).reshape(PIECES, LANES)
        grad4 = grad_out.reshape(n_cp, n, seq_loc, D)
        w_full, small, tok, grads = gather_all(rows_pad(w_loc), small, tokens.reshape(n_cp, n, seq_loc), grad4)
        w_full = w_full.reshape(DX, NQKV)
        small = small.reshape(n_fsdp, PIECES * LANES)
        vecs = small[:, :9 * PV].reshape(n_fsdp, 9, PV).transpose(1, 0, 2).reshape(9, D)
        bup = small[:, 9 * PV:9 * PV + FV].reshape(F, 1)
        tok = tok.transpose(1, 0, 2).reshape(n, 1, S)
        lens = lax.dynamic_slice(lengths, (cp_index * n,), (n,))
        table_t = jnp.pad(embed_table, ((0, VP - embed_table.shape[0]), (0, 0))).T
        vec_cols = jnp.concatenate([vecs[:2], vecs[5:], jnp.zeros((2, D), jnp.float32)], axis=0).T
        slot = np.arange(QP) % HP
        pad_one = jnp.asarray(np.stack([slot == HP - 1, slot >= HALF + ROT]).astype(np.float32))
        bias = jnp.concatenate([(pad_heads(vecs[2:4].reshape(2, H, HD)) + pad_one).reshape(2 * QP), vecs[4]])[:, None]
        rope = jnp.asarray(rope_tables())

        shared = [per_seq((1, S)), const((D, VP)), const((D, 8))]
        rope_spec = const(rope.shape)
        acts = [((QP, S), b16), ((QP, S), b16), ((S, QP), b16), ((S, QP), b16), ((D, S), f32), ((24, S), f32)]
        act_specs = [per_seq(shape) for shape, _ in acts]
        fwd = call(
            attn_fwd_kernel, 3, n,
            shared + [const((NQKV, 1)), rope_spec, const((DX, NQKV))] + anys(5),
            act_specs + anys(4),
            [kind(n, *shape) for shape, kind in acts] + [b16(PIECES, PR, D), b16(PIECES, PR, F), b16(PIECES, FV, D), b16(n_cp, n, seq_loc, D)],
            [bv(NQKV, DX), bv(QP, S), sv(D, S), sv(DX, S)] + [dma(3, PIECES)] * 2 + [dma(QUARTERS)] * 3,
            int(2e10), "attn_fwd", {11: 9})(lens, tok, table_t, vec_cols, bias, rope, w_full, rows_pad(w_out), rows_pad(w_up), w_down, grad4, grads)
        acts, (out_w, up_w, down_w, grads) = fwd[:6], fwd[6:]
        out_w, up_w, down_w = out_w.reshape(DX, D), up_w.reshape(DX, F), down_w.reshape(F, D)
        d_res, dwd, dwu, sv2, layer_out = call(
            ffn_kernel, 4, n,
            shared + [const((F, 1)), per_seq((D, S)), pl.BlockSpec((n_cp, 1, seq_loc, D), lambda i, *_: (0, i, 0, 0)), const((DX, D)), const((DX, F)), const((F, D))],
            [per_seq((D, S)), const((PIECES, FR, D)), const((DX, F)), const((8, D))] + anys(1),
            [f32(n, D, S), f32(PIECES, FR, D), f32(DX, F), f32(8, D), b16(n_seq, seq_loc, D)],
            [bv(D, DX), bv(F, DX), bv(D, F), bv(F, S), bv(F, S), sv(F, LANES), sv(4, D, LANES), sv(D, S), sv(DX, S), sv(DX, S), bv(2, S, D)]
            + [dma(n, QUARTERS)] * 2 + [dma(n)],
            int(4e10), "ffn")(lens, tok, table_t, vec_cols, bup, acts[4], grads, out_w, up_w, down_w)
        ffn_parts = [(r, sl.stop - sl.start) for r, splits in zip((FR, PR), FFN_SPLITS) for sl in splits]
        cut = lambda z: z.reshape(PIECES, PR, z.shape[1])
        dwo, dw, smalls, d_down_w, d_up_w = call(
            attn_bwd_kernel, 5, n,
            shared + [rope_spec] + act_specs + [per_seq((D, S)), const((DX, D)), const((DX, NQKV)), const((8, D))] + anys(2),
            [const((DX, D)), const((DX, 3 * D)), const((HALF + VP, D)), const((FV, D)), const((PV, F))],
            [f32(DX, D), f32(DX, 3 * D), f32(HALF + VP, D), f32(FV, D), f32(PV, F)],
            [bv(QP, S), sv(QP, S), sv(QP, S), sv(NQKV, S), sv(3 * D, S), bv(NQKV, S), sv(3 * D, LANES), sv(2, D, LANES), sv(VP, D), sv(D, S), sv(DX, S), sv(DX, S)]
            + unit_scratch(ffn_parts) + [dma(4, QUARTERS * STAGES)] * 2 + [dma(4, QUARTERS)],
            int(5e10), "attn_bwd")(lens, tok, table_t, vec_cols, rope, *acts, d_res, out_w, w_full, sv2, dwd, cut(dwu))
        d_qkv, d_out_w, smalls = reduce_all(cut(dw), cut(dwo), smalls)
        d_qkv = d_qkv.reshape((PV,) + w_qkv.shape[1:])
        all_vecs = jnp.concatenate([smalls[8:13], smalls[4:8]], axis=0)
        d_vecs = lax.dynamic_slice(all_vecs, (0, f_index * PV), (9, PV))
        d_bup = lax.dynamic_slice(smalls[:4].reshape(F), (f_index * FV,), (FV,))
        return layer_out, smalls[HALF:HALF + embed_table.shape[0]], d_vecs, d_qkv, d_out_w, d_up_w, d_bup, d_down_w

    rows = P('fsdp', None)
    in_specs = (P('fsdp', 'cp'), P('fsdp'), P(), P(None, 'fsdp'), P('fsdp', None, None, None), rows, rows, P('fsdp'), rows, P('fsdp', 'cp', None))
    out_specs = (P('fsdp', 'cp', None), P(), P(None, 'fsdp'), P('fsdp', None, None, None), rows, rows, P('fsdp'), rows)
    return jax.shard_map(local_step, mesh=mesh, in_specs=in_specs, out_specs=out_specs, check_vma=False)
```
